256 devices in a mesh: row: 64 (over z, y, core), col: 4 (over x).
Axes of the slice: x: 4, y: 4, z: 8, core: 2. Of those that a mesh axis runs over, the one named last changes fastest.
Arguments:
- pair_act: bfloat16 [768, 768, 128], P('row', 'col'), may hold values from -6 to 6
- tile_mask: int32 [12, 12], replicated, may hold values 0 or 1
- w_left_gate: bfloat16 [128, 128], replicated, may hold values from -0.5 to 0.5
- w_left: bfloat16 [128, 128], replicated, may hold values from -0.5 to 0.5
- w_right_gate: bfloat16 [128, 128], replicated, may hold values from -0.5 to 0.5
- w_right: bfloat16 [128, 128], replicated, may hold values from -0.5 to 0.5
- w_out_gate: bfloat16 [128, 128], replicated, may hold values from -0.5 to 0.5
- w_out: bfloat16 [128, 128], replicated, may hold values from -0.5 to 0.5
Outputs:
- update: bfloat16 [768, 768, 128], P('row', 'col')
The draws below stay inside these ranges and needn't reach their ends.
All inputs are finite; a program needn't handle non-finite values.
Results may differ from the reference program's by a relative error of at most 0.0083.
Values may be sent and summed in bfloat16 or wider, within the bound.
A program may use at most 64 MiB of HBM per device.

```python
import jax
import jax.numpy as jnp
from jax import lax

CZ = 128
CH = 128
TILES = 12
RES = 768
TILE = 64


def with_ends(result, stream_key, least, largest):
    extent = result.shape
    spot = [jax.random.randint(jax.random.fold_in(stream_key, axis), (), 0, extent[axis]) for axis in range(len(extent))]
    result = result.at[tuple(spot)].set(least)
    longest = extent.index(max(extent))
    spot[longest] = (spot[longest] + 1) % extent[longest]
    return result.at[tuple(spot)].set(largest)


def block_scale(own_key, extent, cuts, low, largest):
    gain, own = 1.0, jax.random.fold_in(own_key, 6)
    for position, shards_of in cuts:
        steps = jnp.exp(jax.random.uniform(jax.random.fold_in(own, position), (shards_of,), jnp.float32, low / len(cuts), largest / len(cuts)))
        gain = gain * jnp.repeat(steps, extent[position] // shards_of).reshape([-1 if axis == position else 1 for axis in range(len(extent))])
    return gain


def normal_values(key, shape, scale, most, cuts=(), kind=jnp.bfloat16):
    entries = scale * jax.random.normal(key, shape, jnp.float32)
    if cuts:
        entries = entries * block_scale(key, shape, cuts, -0.22, 0.18)
    return jnp.clip(entries, -most, most).astype(kind)


def setup_inputs(seed: int = 0) -> dict:
    arg_keys = jax.random.split(jax.random.key(seed), 9)
    return {
        "pair_act": normal_values(arg_keys[0], (RES, RES, CZ), 1.0, 6.0, ((0, 64), (1, 4))),
        "tile_mask": with_ends((jax.random.randint(arg_keys[1], (TILES, TILES), 0, 4) < 3).astype(jnp.int32), jax.random.fold_in(arg_keys[1], 1), 0, 1),
        "w_left_gate": normal_values(arg_keys[2], (CZ, CH), CZ ** -0.5, 0.5),
        "w_left": normal_values(arg_keys[3], (CZ, CH), CZ ** -0.5, 0.5),
        "w_right_gate": normal_values(arg_keys[4], (CZ, CH), CZ ** -0.5, 0.5),
        "w_right": normal_values(arg_keys[5], (CZ, CH), CZ ** -0.5, 0.5),
        "w_out_gate": normal_values(arg_keys[6], (CZ, CZ), CZ ** -0.5, 0.5),
        "w_out": normal_values(arg_keys[7], (CH, CZ), CH ** -0.5, 0.5),
    }


group_width = 8

def norm_last(values):
    mean = lax.optimization_barrier(jnp.mean(values, axis=-1, keepdims=True))
    centred = values - mean
    spread = lax.optimization_barrier(jnp.mean(centred * centred, axis=-1, keepdims=True))
    return centred * lax.rsqrt(spread + 1e-05)

def grouped(weight):
    return weight.reshape(CZ, CH // group_width, group_width).transpose(1, 0, 2)

def reference(pair_act, tile_mask, w_left_gate, w_left, w_right_gate, w_right, w_out_gate, w_out):
    normed = norm_last(pair_act.astype(jnp.float32)).astype(jnp.bfloat16)
    normed_f = lax.optimization_barrier(normed).astype(jnp.float32)
    tile_ids = jnp.arange(RES, dtype=jnp.int32) // TILE
    hot = (tile_ids[:, None] == jnp.arange(TILES, dtype=jnp.int32)[None, :]).astype(jnp.float32)
    pair_mask = jnp.dot(jnp.dot(hot, tile_mask.astype(jnp.float32), preferred_element_type=jnp.float32), hot.T, preferred_element_type=jnp.float32)

    def channel_group(weights):
        left_gate, left_value, right_gate, right_value = weights
        left = jax.nn.sigmoid(jnp.einsum('ikd,de->eik', normed_f, left_gate.astype(jnp.float32)))
        left = (left * jnp.einsum('ikd,de->eik', normed_f, left_value.astype(jnp.float32)) * pair_mask[None]).astype(jnp.bfloat16)
        right = jax.nn.sigmoid(jnp.einsum('jkd,de->ejk', normed_f, right_gate.astype(jnp.float32)))
        right = (right * jnp.einsum('jkd,de->ejk', normed_f, right_value.astype(jnp.float32)) * pair_mask[None]).astype(jnp.bfloat16)
        left_f = lax.optimization_barrier(left).astype(jnp.float32)
        right_f = lax.optimization_barrier(right).astype(jnp.float32)
        return jnp.einsum('cik,cjk->cij', left_f, right_f).astype(jnp.bfloat16)
    triangle = lax.map(channel_group, (grouped(w_left_gate), grouped(w_left), grouped(w_right_gate), grouped(w_right)))
    triangle = triangle.reshape(CH, RES, RES)
    triangle_f = jnp.transpose(lax.optimization_barrier(triangle), (1, 2, 0)).astype(jnp.float32)
    scaled = norm_last(triangle_f).astype(jnp.bfloat16)
    scaled_f = lax.optimization_barrier(scaled).astype(jnp.float32)
    projected = jnp.einsum('ijc,ce->ije', scaled_f, w_out.astype(jnp.float32))
    gate = jax.nn.sigmoid(jnp.einsum('ijd,de->ije', normed_f, w_out_gate.astype(jnp.float32)))
    return (gate * projected).astype(jnp.bfloat16)
```

```python
import functools

import jax
import jax.numpy as jnp
from jax import lax
from jax.experimental import pallas as pl
from jax.experimental.pallas import tpu as pltpu
from jax.sharding import PartitionSpec as P

MESH = pl.DeviceIdType.MESH
NX, NY, NZ, NS, NC = 4, 4, 8, 32, 128
ROWS, COLS, WIDTH = 12, 192, 128
F32, BF16 = jnp.float32, jnp.bfloat16


def unit_norm(values, axis):
    mean = jnp.mean(values, axis=axis, keepdims=True)
    centred = values - mean
    spread = jnp.mean(centred * centred, axis=axis, keepdims=True)
    return centred * lax.rsqrt(spread + 1e-05)


def kernel(
    x_ref, tm_ref, wlg_ref, wl_ref, wrg_ref, wr_ref, wog_ref, wo_ref, out_ref,
    wt, normed, gate, stage, msg, r_own, r_all, l_own, t_odd, t_a, t_b, t_in,
    send_sem, r_sem, l_sem, t_sem, swap_sem, swap_send, local_sem, line_y, line_z,
):
    row, q = lax.axis_index("row"), lax.axis_index("col")
    core, y, z = row % 2, (row // 2) % NY, row // (2 * NY)
    s = row // 2
    chip = s * NX + q
    other = ((s * 2) + 1 - core, q)

    def at(zz, yy, xx):
        return ((zz * NY + yy) * 2 + core, xx)

    x_line = [at(z, y, (q + d) % NX) for d in range(1, NX)]
    y_line = [at(z, (y + d) % NY, q) for d in range(1, NY)]
    z_line = [at((z + d) % NZ, y, q) for d in range(1, NZ)]
    barrier = pltpu.get_barrier_semaphore()
    for peer in [other, *x_line, *y_line, *z_line]:
        pl.semaphore_signal(barrier, inc=1, device_id=peer, device_id_type=MESH)

    for n, w in enumerate((wlg_ref, wl_ref, wrg_ref, wr_ref)):
        wt[n * WIDTH : (n + 1) * WIDTH, :] = w[...].astype(F32).T.astype(BF16)
    low = lax.broadcasted_iota(jnp.int32, (WIDTH, 128), 1) < 64
    odd_q = q % 2 == 1

    def pair_of_rows(p, _):
        parts = {}
        for e in range(2):
            i = 2 * p + e
            n = unit_norm(x_ref[i].astype(F32), 1)
            normed[i] = n.astype(BF16)
            tile = (row * ROWS + i) // 64
            for t in range(3):
                m = tm_ref[tile, q * 3 + t].astype(F32)
                parts[e, t] = (n[t * 64 : (t + 1) * 64] * m).astype(BF16)
        rhs = jnp.concatenate(
            [parts[0, 0], parts[0, 1], parts[1, 0], parts[1, 1], parts[0, 2], parts[1, 2]], axis=0
        )

        def project(n):
            return lax.dot_general(
                wt[n * WIDTH : (n + 1) * WIDTH, :], rhs, (((1,), (1,)), ((), ())),
                preferred_element_type=F32,
            )

        left = jax.nn.sigmoid(project(0)) * project(1)
        right = jax.nn.sigmoid(project(2)) * project(3)
        first = jnp.where(odd_q, right[:, 256:], left[:, 256:])
        second = jnp.where(odd_q, left[:, 256:], right[:, 256:])
        mixed = (
            jnp.where(low, first, pltpu.roll(second, 64, 1)),
            jnp.where(low, pltpu.roll(first, 64, 1), second),
        )
        for e in range(2):
            lanes = slice(e * 128, (e + 1) * 128)
            i = 2 * p + e
            stage[pl.ds(i, NC, stride=36), :] = right[:, lanes]
            stage[pl.ds(12 + i, NC, stride=36), :] = mixed[e]
            stage[pl.ds(24 + i, NC, stride=36), :] = left[:, lanes]
        return 0

    lax.fori_loop(0, ROWS // 2, pair_of_rows, 0)
    flat = msg.reshape(NC * 36, 128)

    def pack(n, _):
        rows = pl.ds(pl.multiple_of(n * 288, 288), 288)
        flat[rows, :] = stage[rows, :].astype(BF16)
        return 0

    lax.fori_loop(0, 16, pack, 0)

    pl.semaphore_wait(barrier, 1 + 3 + 3 + 7)
    for peer in y_line:
        pl.semaphore_signal(line_y, inc=1, device_id=peer, device_id_type=MESH)
    pl.semaphore_wait(line_y, 3)
    for peer in z_line:
        pl.semaphore_signal(line_z, inc=1, device_id=peer, device_id_type=MESH)
    pl.semaphore_wait(line_z, 7)

    def peer_of(o):
        dx, dy, dz = o % NX, (o // NX) % NY, (NZ // 2 + o // (NX * NY)) % NZ
        zz, yy, xx = (z + dz) % NZ, (y + dy) % NY, (q + dx) % NX
        return zz * NY + yy, xx

    me = 64

    def to_all(start):
        def body(o, _):
            start(*peer_of(o))
            return 0

        lax.fori_loop(0, me, body, 0)
        lax.fori_loop(me + 1, NC, body, 0)

    def send_r(ss, xx):
        pltpu.make_async_remote_copy(
            msg.at[ss * NX + xx, pl.ds(0, 2)], r_own.at[:, q, s], send_sem, r_sem,
            device_id=(ss * 2 + core, xx), device_id_type=MESH,
        ).start()

    def send_l(ss, xx):
        pltpu.make_async_remote_copy(
            msg.at[ss * NX + xx, 2], l_own.at[q, s], send_sem, l_sem,
            device_id=(ss * 2 + core, xx), device_id_type=MESH,
        ).start()

    to_all(send_r)
    to_all(send_l)
    own_r = pltpu.make_async_copy(msg.at[chip, pl.ds(0, 2)], r_own.at[:, q, s], local_sem.at[0])
    own_l = pltpu.make_async_copy(msg.at[chip, 2], l_own.at[q, s], local_sem.at[1])
    own_r.start()
    own_l.start()

    def gates(i, _):
        gate[i] = jax.nn.sigmoid(
            jnp.dot(normed[i], wog_ref[...], preferred_element_type=F32)
        )
        return 0

    lax.fori_loop(0, ROWS, gates, 0)

    own_r.wait()
    own_l.wait()
    every = msg.at[pl.ds(0, NC - 1), pl.ds(0, 2)]
    pltpu.make_async_copy(every, every, r_sem).wait()
    swap = pltpu.make_async_remote_copy(
        r_own, r_all.at[:, :, :, core], swap_send, swap_sem, device_id=other, device_id_type=MESH
    )
    swap.start()
    keep = pltpu.make_async_copy(r_own, r_all.at[:, :, :, core], local_sem.at[2])
    keep.start()
    every = msg.at[pl.ds(0, NC - 1), 2]
    pltpu.make_async_copy(every, every, l_sem).wait()
    keep.wait()
    swap.wait()

    la = l_own.reshape(NX * 384, 128)
    ra = r_all.reshape(2 * NX * 768, 128)
    rb = r_own.reshape(2 * NX * 384, 128)

    def block(ref, n, size):
        return ref[n * size : (n + 1) * size, :]

    lhs = [block(la, x, 384) for x in range(NX)]
    rhs = [block(ra, x, 768) for x in range(NX)]
    for x in (0, 2):
        lhs.append(
            jnp.concatenate(
                [block(rb, NX + x, 384)[:, :64], block(rb, NX + x + 1, 384)[:, 64:]], axis=1
            )
        )
        rhs.append(
            jnp.concatenate(
                [block(ra, NX + x, 768)[:, 64:], block(ra, NX + x + 1, 768)[:, :64]], axis=1
            )
        )
    triangle = lax.dot_general(
        jnp.concatenate(lhs, axis=1), jnp.concatenate(rhs, axis=1), (((1,), (1,)), ((), ())),
        preferred_element_type=F32,
    )
    whole = t_a.reshape(NX * 384, 128)
    halves = t_b.reshape(NX * 192, 128)
    lane_b = lax.broadcasted_iota(jnp.int32, (192, 128), 1) < 64
    for x, tile in enumerate((0, 2, 3, 5)):
        whole[x * 384 : (x + 1) * 384, :] = triangle[:, tile * 128 : (tile + 1) * 128].astype(BF16)
    for n, tile in enumerate((1, 4)):
        t_odd[...] = triangle[:, tile * 128 : (tile + 1) * 128]
        even, odd = t_odd[pl.ds(0, 192, stride=2), :], t_odd[pl.ds(1, 192, stride=2), :]
        b0 = jnp.where(lane_b, even, pltpu.roll(odd, 64, 1))
        b1 = jnp.where(lane_b, pltpu.roll(even, 64, 1), odd)
        halves[(2 * n) * 192 : (2 * n + 1) * 192, :] = b0.astype(BF16)
        halves[(2 * n + 1) * 192 : (2 * n + 2) * 192, :] = b1.astype(BF16)

    def send_t(ss, xx):
        for src, dst in ((t_a, pl.ds(0, 6)), (t_b, pl.ds(6, 3))):
            pltpu.make_async_remote_copy(
                src.at[xx, ss], t_in.at[chip, dst], send_sem, t_sem,
                device_id=(ss * 2 + core, xx), device_id_type=MESH,
            ).start()

    to_all(send_t)
    own_a = pltpu.make_async_copy(t_a.at[q, s], t_in.at[chip, pl.ds(0, 6)], local_sem.at[0])
    own_b = pltpu.make_async_copy(t_b.at[q, s], t_in.at[chip, pl.ds(6, 3)], local_sem.at[1])
    own_a.start()
    own_b.start()
    own_a.wait()
    own_b.wait()
    every = t_in.at[pl.ds(0, NC - 1)]
    pltpu.make_async_copy(every, every, t_sem).wait()

    flat_t = t_in.reshape(NC * 18, 128)

    def unpack(n, _):
        rows = pl.ds(pl.multiple_of(n * 288, 288), 288)
        stage[rows, :] = flat_t[rows, :].astype(F32)
        return 0

    lax.fori_loop(0, 8, unpack, 0)

    def projected(g):
        scaled = unit_norm(stage[pl.ds(g, NC, stride=18), :], 0)
        return jnp.dot(scaled.T.astype(BF16), wo_ref[...], preferred_element_type=F32)

    a0 = pl.multiple_of((q % 2) * 64, 64)
    b0 = pl.multiple_of((1 - q % 2) * 128, 128)

    def whole_rows(i, _):
        out_ref[i, pl.ds(a0, 128), :] = (gate[i, pl.ds(a0, 128), :] * projected(i)).astype(BF16)
        return 0

    def half_rows(p, _):
        both = projected(12 + p)
        for e in range(2):
            out_ref[2 * p + e, pl.ds(b0, 64), :] = (
                gate[2 * p + e, pl.ds(b0, 64), :] * both[e * 64 : (e + 1) * 64]
            ).astype(BF16)
        return 0

    lax.fori_loop(0, 12, whole_rows, 0)
    lax.fori_loop(0, 6, half_rows, 0)
    sent = msg.at[pl.ds(0, NC - 1)]
    pltpu.make_async_copy(sent, sent, send_sem).wait()
    sent = t_in.at[pl.ds(0, NC - 1)]
    pltpu.make_async_copy(sent, sent, send_sem).wait()


def local(*args):
    vmem = pl.BlockSpec(memory_space=pltpu.VMEM)
    smem = pl.BlockSpec(memory_space=pltpu.SMEM)
    dma = pltpu.SemaphoreType.DMA
    return pl.pallas_call(
        kernel,
        out_shape=jax.ShapeDtypeStruct((ROWS, COLS, WIDTH), BF16),
        in_specs=[vmem, smem] + [vmem] * 6,
        out_specs=vmem,
        scratch_shapes=[
            pltpu.VMEM((4 * WIDTH, WIDTH), BF16),
            pltpu.VMEM((ROWS, COLS, WIDTH), BF16),
            pltpu.VMEM((ROWS, COLS, WIDTH), F32),
            pltpu.VMEM((NC * 36, 128), F32),
            pltpu.VMEM((NC, 3, 3, 4, 128), BF16),
            pltpu.VMEM((2, NX, NS, 3, 4, 128), BF16),
            pltpu.VMEM((2, NX, NS, 2, 3, 4, 128), BF16),
            pltpu.VMEM((NX, NS, 3, 4, 128), BF16),
            pltpu.VMEM((384, 128), F32),
            pltpu.VMEM((NX, NS, 6, 2, 128), BF16),
            pltpu.VMEM((NX, NS, 3, 2, 128), BF16),
            pltpu.VMEM((NC, 9, 2, 128), BF16),
            dma, dma, dma, dma, dma, dma, pltpu.SemaphoreType.DMA((3,)),
            pltpu.SemaphoreType.REGULAR, pltpu.SemaphoreType.REGULAR,
        ],
        compiler_params=pltpu.CompilerParams(
            collective_id=0, has_side_effects=True, vmem_limit_bytes=48 * 2**20
        ),
    )(*args)


def solution(mesh):
    return jax.shard_map(
        local,
        mesh=mesh,
        in_specs=(P("row", "col", None), P(), P(), P(), P(), P(), P(), P()),
        out_specs=P("row", "col", None),
        check_vma=False,
    )
```

```python
import functools

import jax
import jax.numpy as jnp
from jax import lax
from jax.experimental import pallas as pl
from jax.experimental.pallas import tpu as pltpu
from jax.sharding import PartitionSpec as P

MESH = pl.DeviceIdType.MESH
NX, NY, NZ, NS, NC = 4, 4, 8, 32, 128
ROWS, COLS, WIDTH = 12, 192, 128
F32, BF16 = jnp.float32, jnp.bfloat16
UNROLL = 3


def unit_norm(values, axis):
    mean = jnp.mean(values, axis=axis, keepdims=True)
    centred = values - mean
    spread = jnp.mean(centred * centred, axis=axis, keepdims=True)
    return centred * lax.rsqrt(spread + 1e-05)


def kernel(
    x_hbm, tm_hbm, wlg_hbm, wl_hbm, wrg_hbm, wr_hbm, wog_hbm, wo_hbm, out_ref,
    x_ref, tm_ref, w_in, wt, normed, gate, stage, msg, r_own, r_all, r_mix, l_own, t_odd, t_a, t_b,
    in_a, in_b, load_sem, send_sem, r_sem, l_sem, a_sem, b_sem, swap_sem, swap_send, keep_sem,
    line_y, line_x,
):
    row, q = lax.axis_index("row"), lax.axis_index("col")
    core, y, z = row % 2, (row // 2) % NY, row // (2 * NY)
    s = row // 2
    chip = s * NX + q
    other = ((s * 2) + 1 - core, q)

    loads = [
        [
            pltpu.make_async_copy(w, w_in.at[n], load_sem.at[0])
            for n, w in enumerate((wlg_hbm, wl_hbm, wrg_hbm, wr_hbm, wog_hbm, wo_hbm))
        ],
        [pltpu.make_async_copy(tm_hbm, tm_ref, load_sem.at[1])],
    ] + [
        [pltpu.make_async_copy(x_hbm.at[pl.ds(4 * n, 4)], x_ref.at[pl.ds(4 * n, 4)], load_sem.at[2 + n])]
        for n in range(3)
    ]
    for load in loads:
        for copy in load:
            copy.start()

    def at(zz, yy, xx):
        return ((zz * NY + yy) * 2 + core, xx)

    x_line = [at(z, y, (q + d) % NX) for d in range(1, NX)]
    y_line = [at(z, (y + d) % NY, q) for d in range(1, NY)]
    z_line = [at((z + d) % NZ, y, q) for d in range(1, NZ)]
    barrier = pltpu.get_barrier_semaphore()
    for peer in [*z_line, other, *x_line, *y_line]:
        pl.semaphore_signal(barrier, inc=1, device_id=peer, device_id_type=MESH)

    pltpu.make_async_copy(w_in, w_in, load_sem.at[0]).wait()
    for n in range(4):
        wt[n * WIDTH : (n + 1) * WIDTH, :] = w_in[n].astype(F32).T.astype(BF16)
    low = lax.broadcasted_iota(jnp.int32, (WIDTH, 128), 1) < 64
    odd_q = q % 2 == 1
    loads[1][0].wait()

    def pair_of_rows(p, _):
        parts = {}
        for e in range(2):
            i = 2 * p + e
            n = unit_norm(x_ref[i].astype(F32), 1)
            normed[i] = n.astype(BF16)
            tile = (row * ROWS + i) // 64
            for t in range(3):
                m = tm_ref[tile, q * 3 + t].astype(F32)
                parts[e, t] = (n[t * 64 : (t + 1) * 64] * m).astype(BF16)
        rhs = jnp.concatenate(
            [parts[0, 0], parts[0, 1], parts[1, 0], parts[1, 1], parts[0, 2], parts[1, 2]], axis=0
        )

        def project(n):
            return lax.dot_general(
                wt[n * WIDTH : (n + 1) * WIDTH, :], rhs, (((1,), (1,)), ((), ())),
                preferred_element_type=F32,
            )

        left = jax.nn.sigmoid(project(0)) * project(1)
        right = jax.nn.sigmoid(project(2)) * project(3)
        first = jnp.where(odd_q, right[:, 256:], left[:, 256:])
        second = jnp.where(odd_q, left[:, 256:], right[:, 256:])
        mixed = (
            jnp.where(low, first, pltpu.roll(second, 64, 1)),
            jnp.where(low, pltpu.roll(first, 64, 1), second),
        )
        for e in range(2):
            lanes = slice(e * 128, (e + 1) * 128)
            i = 2 * p + e
            stage[pl.ds(i, NC, stride=36), :] = right[:, lanes]
            stage[pl.ds(12 + i, NC, stride=36), :] = mixed[e]
            stage[pl.ds(24 + i, NC, stride=36), :] = left[:, lanes]
        return 0

    loads[2][0].wait()
    lax.fori_loop(0, 2, pair_of_rows, 0)
    pl.semaphore_wait(barrier, 1 + 3 + 3 + 7)
    for peer in y_line:
        pl.semaphore_signal(line_y, inc=1, device_id=peer, device_id_type=MESH)
    loads[3][0].wait()
    lax.fori_loop(2, 4, pair_of_rows, 0)
    pl.semaphore_wait(line_y, 3)
    for peer in x_line:
        pl.semaphore_signal(line_x, inc=1, device_id=peer, device_id_type=MESH)
    loads[4][0].wait()
    lax.fori_loop(4, 6, pair_of_rows, 0)
    flat = msg.reshape(NC * 36, 128)

    def pack(n, _):
        rows = pl.ds(pl.multiple_of(n * 288, 288), 288)
        flat[rows, :] = stage[rows, :].astype(BF16)
        return 0

    lax.fori_loop(0, 16, pack, 0)
    pl.semaphore_wait(line_x, 3)

    def to_group(k):
        return (z + NZ // 2 + k) % NZ

    def from_group(k):
        return (z + NZ // 2 - k) % NZ

    me = 64

    def to_all(begin, send):
        def one(o, _):
            k = o // 16
            send(k, to_group(k) * NY + (y + (o // NX)) % NY, (q + o) % NX)
            return 0

        lax.fori_loop(begin, me, one, 0)
        lax.fori_loop(me + 1, NC, one, 0)

    def send_r(k, ss, xx):
        pltpu.make_async_remote_copy(
            msg.at[ss * NX + xx, pl.ds(0, 2)], r_own.at[:, q, s], send_sem, r_sem.at[k],
            device_id=(ss * 2 + core, xx), device_id_type=MESH,
        ).start()

    def send_l(k, ss, xx):
        pltpu.make_async_remote_copy(
            msg.at[ss * NX + xx, 2], l_own.at[q, s], send_sem, l_sem.at[k],
            device_id=(ss * 2 + core, xx), device_id_type=MESH,
        ).start()

    pltpu.make_async_copy(msg.at[chip, pl.ds(0, 2)], r_own.at[:, q, s], r_sem.at[4]).start()
    pltpu.make_async_copy(msg.at[chip, 2], l_own.at[q, s], l_sem.at[4]).start()
    to_all(0, send_r)
    to_all(0, send_l)

    def gates(i, _):
        gate[i] = jax.nn.sigmoid(jnp.dot(normed[i], w_in[4], preferred_element_type=F32))
        return 0

    lax.fori_loop(0, ROWS, gates, 0)

    def swap(k, _):
        four = pl.ds(from_group(k) * NY, NY)
        block = r_own.at[:, :, four]
        pltpu.make_async_copy(block, block, r_sem.at[k]).wait()
        pltpu.make_async_remote_copy(
            block, r_all.at[:, :, four, core], swap_send, swap_sem, device_id=other, device_id_type=MESH
        ).start()
        pltpu.make_async_copy(block, r_all.at[:, :, four, core], keep_sem).start()
        return 0

    lax.fori_loop(0, NZ, swap, 0)
    pltpu.make_async_copy(r_own, r_own, keep_sem).wait()
    pltpu.make_async_copy(r_own, r_own, swap_sem).wait()

    ra = r_all.reshape(2 * NX * 768, 128)
    rb = r_own.reshape(2 * NX * 384, 128)
    la = l_own.reshape(NX * 384, 128)
    whole = t_a.reshape(NX * 384, 128)
    halves = t_b.reshape(NX * 192, 128)

    def block(ref, n, size):
        return ref[n * size : (n + 1) * size, :]

    for n, x in enumerate((0, 2)):
        r_mix[n] = jnp.concatenate(
            [block(ra, NX + x, 768)[:, 64:], block(ra, NX + x + 1, 768)[:, :64]], axis=1
        )
    lane_b = lax.broadcasted_iota(jnp.int32, (24, 128), 1) < 64

    def rows_of(k, _):
        zz = from_group(k)
        arrived = msg.at[pl.ds(0, 16), 2]
        pltpu.make_async_copy(arrived, arrived, l_sem.at[k]).wait()

        def part(ref, n):
            return ref[pl.ds(pl.multiple_of(n * 384 + zz * 48, 48), 48), :]

        lhs = [part(la, x) for x in range(NX)]
        for x in (0, 2):
            lhs.append(
                jnp.concatenate([part(rb, NX + x)[:, :64], part(rb, NX + x + 1)[:, 64:]], axis=1)
            )
        rhs = [block(ra, x, 768) for x in range(NX)] + [r_mix[0], r_mix[1]]
        triangle = lax.dot_general(
            jnp.concatenate(lhs, axis=1), jnp.concatenate(rhs, axis=1), (((1,), (1,)), ((), ())),
            preferred_element_type=F32,
        )
        for x, tile in enumerate((0, 2, 3, 5)):
            whole[pl.ds(pl.multiple_of(x * 384 + zz * 48, 48), 48), :] = triangle[
                :, tile * 128 : (tile + 1) * 128
            ].astype(BF16)
        for n, tile in enumerate((1, 4)):
            t_odd[n] = triangle[:, tile * 128 : (tile + 1) * 128]
            even, odd = t_odd[n, pl.ds(0, 24, stride=2), :], t_odd[n, pl.ds(1, 24, stride=2), :]
            b0 = jnp.where(lane_b, even, pltpu.roll(odd, 64, 1))
            b1 = jnp.where(lane_b, pltpu.roll(even, 64, 1), odd)
            halves[pl.ds(pl.multiple_of(2 * n * 192 + zz * 24, 8), 24), :] = b0.astype(BF16)
            halves[pl.ds(pl.multiple_of((2 * n + 1) * 192 + zz * 24, 8), 24), :] = b1.astype(BF16)

        def back(j, _):
            ss, xx = zz * NY + (y + j // NX) % NY, (q + j) % NX

            @pl.when((k != 4) | (j != 0))
            def _():
                pltpu.make_async_remote_copy(
                    t_a.at[xx, ss], in_a.at[chip], send_sem, a_sem,
                    device_id=(ss * 2 + core, xx), device_id_type=MESH,
                ).start()

            return 0

        lax.fori_loop(0, 16, back, 0)
        return 0

    lax.fori_loop(0, NZ, rows_of, 0)
    pltpu.make_async_copy(t_a.at[q, s], in_a.at[chip], a_sem).start()
    pltpu.make_async_copy(t_b.at[q, s], in_b.at[chip], b_sem).start()

    def send_b(k, ss, xx):
        pltpu.make_async_remote_copy(
            t_b.at[xx, ss], in_b.at[chip], send_sem, b_sem,
            device_id=(ss * 2 + core, xx), device_id_type=MESH,
        ).start()

    to_all(0, send_b)

    def unpack(source, steps):
        def some(n, _):
            rows = pl.ds(pl.multiple_of(n * 256, 256), 256)
            stage[rows, :] = source[rows, :].astype(F32)
            return 0

        lax.fori_loop(0, steps, some, 0)

    def projected(g, stride):
        scaled = unit_norm(stage[pl.ds(g, NC, stride=stride), :], 0)
        return jnp.dot(scaled.T.astype(BF16), w_in[5], preferred_element_type=F32)

    a0 = pl.multiple_of((q % 2) * 64, 64)
    b0 = pl.multiple_of((1 - q % 2) * 128, 128)

    def whole_rows(i, _):
        out_ref[i, pl.ds(a0, 128), :] = (gate[i, pl.ds(a0, 128), :] * projected(i, 12)).astype(BF16)
        return 0

    def half_rows(p, _):
        both = projected(p, 6)
        for e in range(2):
            out_ref[2 * p + e, pl.ds(b0, 64), :] = (
                gate[2 * p + e, pl.ds(b0, 64), :] * both[e * 64 : (e + 1) * 64]
            ).astype(BF16)
        return 0

    pltpu.make_async_copy(in_a, in_a, a_sem).wait()
    unpack(in_a.reshape(NC * 12, 128), 6)
    lax.fori_loop(0, 12, whole_rows, 0, unroll=UNROLL)
    pltpu.make_async_copy(in_b, in_b, b_sem).wait()
    unpack(in_b.reshape(NC * 6, 128), 3)
    lax.fori_loop(0, 6, half_rows, 0, unroll=UNROLL)
    for sent in (msg, in_a, in_b):
        sent = sent.at[pl.ds(0, NC - 1)]
        pltpu.make_async_copy(sent, sent, send_sem).wait()
    pltpu.make_async_copy(r_own, r_own, swap_send).wait()


def local(*args):
    hbm = pl.BlockSpec(memory_space=pltpu.HBM)
    vmem = pl.BlockSpec(memory_space=pltpu.VMEM)
    dma = pltpu.SemaphoreType.DMA
    return pl.pallas_call(
        kernel,
        out_shape=jax.ShapeDtypeStruct((ROWS, COLS, WIDTH), BF16),
        in_specs=[hbm] * 8,
        out_specs=vmem,
        scratch_shapes=[
            pltpu.VMEM((ROWS, COLS, WIDTH), BF16),
            pltpu.SMEM((12, 12), jnp.int32),
            pltpu.VMEM((6, WIDTH, WIDTH), BF16),
            pltpu.VMEM((4 * WIDTH, WIDTH), BF16),
            pltpu.VMEM((ROWS, COLS, WIDTH), BF16),
            pltpu.VMEM((ROWS, COLS, WIDTH), F32),
            pltpu.VMEM((NC * 36, 128), F32),
            pltpu.VMEM((NC, 3, 3, 4, 128), BF16),
            pltpu.VMEM((2, NX, NS, 3, 4, 128), BF16),
            pltpu.VMEM((2, NX, NS, 2, 3, 4, 128), BF16),
            pltpu.VMEM((2, 768, 128), BF16),
            pltpu.VMEM((NX, NS, 3, 4, 128), BF16),
            pltpu.VMEM((2, 48, 128), F32),
            pltpu.VMEM((NX, NS, 6, 2, 128), BF16),
            pltpu.VMEM((NX, NS, 3, 2, 128), BF16),
            pltpu.VMEM((NC, 6, 2, 128), BF16),
            pltpu.VMEM((NC, 3, 2, 128), BF16),
            dma((5,)), dma, dma((NZ,)), dma((NZ,)), dma, dma, dma, dma, dma,
            pltpu.SemaphoreType.REGULAR, pltpu.SemaphoreType.REGULAR,
        ],
        compiler_params=pltpu.CompilerParams(
            collective_id=0, has_side_effects=True, vmem_limit_bytes=67043328
        ),
    )(*args)


def solution(mesh):
    return jax.shard_map(
        local,
        mesh=mesh,
        in_specs=(P("row", "col", None), P(), P(), P(), P(), P(), P(), P()),
        out_specs=P("row", "col", None),
        check_vma=False,
    )
```

```python
import functools

import jax
import jax.numpy as jnp
from jax import lax
from jax.experimental import pallas as pl
from jax.experimental.pallas import tpu as pltpu
from jax.sharding import PartitionSpec as P

MESH = pl.DeviceIdType.MESH
NX, NY, NZ, NS, NC = 4, 4, 8, 32, 128
ROWS, COLS, WIDTH = 12, 192, 128
F32, BF16 = jnp.float32, jnp.bfloat16
UNROLL, UNROLL_PREP = 3, 3


def unit_norm(values, axis):
    mean = jnp.mean(values, axis=axis, keepdims=True)
    centred = values - mean
    spread = jnp.mean(centred * centred, axis=axis, keepdims=True)
    return centred * lax.rsqrt(spread + 1e-05)


def kernel(
    x_hbm, tm_hbm, wlg_hbm, wl_hbm, wrg_hbm, wr_hbm, wog_hbm, wo_hbm, out_ref,
    x_ref, tm_ref, w_in, wt, normed, masked, gate, stage, msg_r, msg_l, r_own, r_all, r_mix, l_own,
    t_odd, t_a, t_b, in_a, in_b,
    load_sem, send_sem, r_sem, l_sem, a_sem, b_sem, swap_sem, swap_send, keep_sem, line_y, line_x,
):
    row, q = lax.axis_index("row"), lax.axis_index("col")
    core, y, z = row % 2, (row // 2) % NY, row // (2 * NY)
    s = row // 2
    chip = s * NX + q
    other = ((s * 2) + 1 - core, q)

    weights = (wlg_hbm, wl_hbm, wrg_hbm, wr_hbm, wog_hbm, wo_hbm)
    for n, w in enumerate(weights):
        pltpu.make_async_copy(w, w_in.at[n], load_sem.at[0]).start()
    load_mask = pltpu.make_async_copy(tm_hbm, tm_ref, load_sem.at[1])
    load_mask.start()
    load_x = [
        pltpu.make_async_copy(x_hbm.at[pl.ds(6 * n, 6)], x_ref.at[pl.ds(6 * n, 6)], load_sem.at[2 + n])
        for n in range(2)
    ]
    for load in load_x:
        load.start()

    def at(zz, yy, xx):
        return ((zz * NY + yy) * 2 + core, xx)

    x_line = [at(z, y, (q + d) % NX) for d in range(1, NX)]
    y_line = [at(z, (y + d) % NY, q) for d in range(1, NY)]
    z_line = [at((z + d) % NZ, y, q) for d in (4, 3, 5, 2, 6, 1, 7)]
    barrier = pltpu.get_barrier_semaphore()
    for peer in [*z_line, *y_line, *x_line, other]:
        pl.semaphore_signal(barrier, inc=1, device_id=peer, device_id_type=MESH)

    pltpu.make_async_copy(w_in, w_in, load_sem.at[0]).wait()
    for n in range(4):
        wt[n * WIDTH : (n + 1) * WIDTH, :] = w_in[n].astype(F32).T.astype(BF16)
    low = lax.broadcasted_iota(jnp.int32, (WIDTH, 128), 1) < 64
    odd_q = q % 2 == 1
    load_mask.wait()

    def project(n, values):
        return lax.dot_general(
            wt[n * WIDTH : (n + 1) * WIDTH, :], values, (((1,), (1,)), ((), ())),
            preferred_element_type=F32,
        )

    def right_rows(p, _):
        parts = {}
        for e in range(2):
            i = 2 * p + e
            n = unit_norm(x_ref[i].astype(F32), 1)
            normed[i] = n.astype(BF16)
            tile = (row * ROWS + i) // 64
            for t in range(3):
                m = tm_ref[tile, q * 3 + t].astype(F32)
                parts[e, t] = (n[t * 64 : (t + 1) * 64] * m).astype(BF16)
        firsts = jnp.concatenate([parts[0, 0], parts[0, 1], parts[1, 0], parts[1, 1]], axis=0)
        lasts = jnp.concatenate([parts[0, 2], parts[1, 2]], axis=0)
        masked[p] = firsts
        right = jax.nn.sigmoid(project(2, firsts)) * project(3, firsts)
        right_last = jax.nn.sigmoid(project(2, lasts)) * project(3, lasts)
        left_last = jax.nn.sigmoid(project(0, lasts)) * project(1, lasts)
        first = jnp.where(odd_q, right_last, left_last)
        second = jnp.where(odd_q, left_last, right_last)
        mixed = (
            jnp.where(low, first, pltpu.roll(second, 64, 1)),
            jnp.where(low, pltpu.roll(first, 64, 1), second),
        )
        for e in range(2):
            stage[pl.ds(2 * p + e, NC, stride=24), :] = right[:, e * 128 : (e + 1) * 128]
            stage[pl.ds(12 + 2 * p + e, NC, stride=24), :] = mixed[e]
        return 0

    def left_rows(p, _):
        left = jax.nn.sigmoid(project(0, masked[p])) * project(1, masked[p])
        for e in range(2):
            stage[pl.ds(2 * p + e, NC, stride=12), :] = left[:, e * 128 : (e + 1) * 128]
        return 0

    def pack(target, steps):
        def some(n, _):
            rows = pl.ds(pl.multiple_of(n * 256, 256), 256)
            target[rows, :] = stage[rows, :].astype(BF16)
            return 0

        lax.fori_loop(0, steps, some, 0)

    load_x[0].wait()
    lax.fori_loop(0, 3, right_rows, 0, unroll=UNROLL_PREP)
    pl.semaphore_wait(barrier, 1 + 3 + 3 + 7)
    for peer in y_line:
        pl.semaphore_signal(line_y, inc=1, device_id=peer, device_id_type=MESH)
    load_x[1].wait()
    lax.fori_loop(3, 6, right_rows, 0, unroll=UNROLL_PREP)
    pack(msg_r.reshape(NC * 24, 128), 12)
    pl.semaphore_wait(line_y, 3)
    for peer in x_line:
        pl.semaphore_signal(line_x, inc=1, device_id=peer, device_id_type=MESH)

    def send_r(dx, k, dy):
        dz = 4 + ((k + 1) // 2) * (1 - 2 * (k % 2))
        ss, xx = ((z + dz) % NZ) * NY + (y + dy) % NY, (q + dx) % NX
        pltpu.make_async_remote_copy(
            msg_r.at[ss * NX + xx], r_own.at[:, q, s], send_sem, r_sem.at[dx],
            device_id=(ss * 2 + core, xx), device_id_type=MESH,
        ).start()
        return 0

    pltpu.make_async_copy(msg_r.at[chip], r_own.at[:, q, s], r_sem.at[0]).start()
    lax.fori_loop(0, 7, lambda o, _: send_r(0, o, 0), 0)
    lax.fori_loop(0, 24, lambda o, _: send_r(0, o // 3, 1 + o % 3), 0)
    pl.semaphore_wait(line_x, 3)
    lax.fori_loop(32, NC, lambda o, _: send_r(o // 32, (o // 4) % 8, o % 4), 0)

    lax.fori_loop(0, 6, left_rows, 0, unroll=UNROLL_PREP)
    pack(msg_l.reshape(NC * 12, 128), 6)

    def offset(g, e):
        return 4 - g if e == 0 else 4 + g + 4 * ((3 - g) // 3)

    def target(o):
        g, e = o // 32, o % 2
        dz = (4 - g) + e * (2 * g + 4 * ((3 - g) // 3))
        return ((z + dz) % NZ) * NY + (y + (o // 8)) % NY, (q + o // 2) % NX

    me = 1

    def to_all(send):
        send(0)
        lax.fori_loop(me + 1, NC, lambda o, _: send(o), 0)

    def send_l(o):
        ss, xx = target(o)
        pltpu.make_async_remote_copy(
            msg_l.at[ss * NX + xx], l_own.at[q, s], send_sem, l_sem.at[o // 32],
            device_id=(ss * 2 + core, xx), device_id_type=MESH,
        ).start()
        return 0

    pltpu.make_async_copy(msg_l.at[chip], l_own.at[q, s], l_sem.at[0]).start()
    to_all(send_l)

    def gates(i, _):
        gate[i] = jax.nn.sigmoid(jnp.dot(normed[i], w_in[4], preferred_element_type=F32))
        return 0

    lax.fori_loop(0, ROWS, gates, 0)

    def swap(dx, _):
        block = r_own.at[:, (q + NX - dx) % NX]
        mine = r_all.at[:, (q + NX - dx) % NX, :, core]
        pltpu.make_async_copy(block, block, r_sem.at[dx]).wait()
        pltpu.make_async_remote_copy(
            block, mine, swap_send, swap_sem, device_id=other, device_id_type=MESH
        ).start()
        pltpu.make_async_copy(block, mine, keep_sem).start()
        return 0

    lax.fori_loop(0, NX, swap, 0)
    pltpu.make_async_copy(r_own, r_own, keep_sem).wait()
    pltpu.make_async_copy(r_own, r_own, swap_sem).wait()

    ra = r_all.reshape(2 * NX * 768, 128)
    rb = r_own.reshape(2 * NX * 384, 128)
    la = l_own.reshape(NX * 384, 128)
    whole = t_a.reshape(NX * 384, 128)
    halves = t_b.reshape(NX * 192, 128)

    def block(ref, n, size):
        return ref[n * size : (n + 1) * size, :]

    for n, x in enumerate((0, 2)):
        r_mix[n] = jnp.concatenate(
            [block(ra, NX + x, 768)[:, 64:], block(ra, NX + x + 1, 768)[:, :64]], axis=1
        )
    lane_b = lax.broadcasted_iota(jnp.int32, (48, 128), 1) < 64

    def rows_of(g, _):
        places = [(z + NZ - offset(g, e)) % NZ for e in range(2)]
        arrived = msg_l.at[pl.ds(0, 32)]
        pltpu.make_async_copy(arrived, arrived, l_sem.at[g]).wait()

        def part(ref, n):
            return jnp.concatenate(
                [ref[pl.ds(pl.multiple_of(n * 384 + zz * 48, 48), 48), :] for zz in places], axis=0
            )

        lhs = [part(la, x) for x in range(NX)]
        for x in (0, 2):
            lhs.append(
                jnp.concatenate([part(rb, NX + x)[:, :64], part(rb, NX + x + 1)[:, 64:]], axis=1)
            )
        rhs = [block(ra, x, 768) for x in range(NX)] + [r_mix[0], r_mix[1]]
        triangle = lax.dot_general(
            jnp.concatenate(lhs, axis=1), jnp.concatenate(rhs, axis=1), (((1,), (1,)), ((), ())),
            preferred_element_type=F32,
        )
        for e, zz in enumerate(places):
            for x, tile in enumerate((0, 2, 3, 5)):
                whole[pl.ds(pl.multiple_of(x * 384 + zz * 48, 48), 48), :] = triangle[
                    e * 48 : (e + 1) * 48, tile * 128 : (tile + 1) * 128
                ].astype(BF16)

        def back(j, _):
            @pl.when((g != 0) | (j != me))
            def _():
                ss, xx = target(g * 32 + j)
                pltpu.make_async_remote_copy(
                    t_a.at[xx, ss], in_a.at[chip], send_sem, a_sem,
                    device_id=(ss * 2 + core, xx), device_id_type=MESH,
                ).start()

            return 0

        lax.fori_loop(0, 32, back, 0)
        for n, tile in enumerate((1, 4)):
            t_odd[n] = triangle[:, tile * 128 : (tile + 1) * 128]
            even, odd = t_odd[n, pl.ds(0, 48, stride=2), :], t_odd[n, pl.ds(1, 48, stride=2), :]
            both = (
                jnp.where(lane_b, even, pltpu.roll(odd, 64, 1)),
                jnp.where(lane_b, pltpu.roll(even, 64, 1), odd),
            )
            for e, zz in enumerate(places):
                for h in range(2):
                    halves[pl.ds(pl.multiple_of((2 * n + h) * 192 + zz * 24, 8), 24), :] = both[h][
                        e * 24 : (e + 1) * 24
                    ].astype(BF16)
        return 0

    lax.fori_loop(0, 4, rows_of, 0)
    pltpu.make_async_copy(t_a.at[q, s], in_a.at[chip], a_sem).start()
    pltpu.make_async_copy(t_b.at[q, s], in_b.at[chip], b_sem).start()

    def send_b(o):
        ss, xx = target(o)
        pltpu.make_async_remote_copy(
            t_b.at[xx, ss], in_b.at[chip], send_sem, b_sem,
            device_id=(ss * 2 + core, xx), device_id_type=MESH,
        ).start()
        return 0

    to_all(send_b)

    def unpack(source, steps):
        def some(n, _):
            rows = pl.ds(pl.multiple_of(n * 256, 256), 256)
            stage[rows, :] = source[rows, :].astype(F32)
            return 0

        lax.fori_loop(0, steps, some, 0)

    def projected(g, stride):
        scaled = unit_norm(stage[pl.ds(g, NC, stride=stride), :], 0)
        return jnp.dot(scaled.T.astype(BF16), w_in[5], preferred_element_type=F32)

    a0 = pl.multiple_of((q % 2) * 64, 64)
    b0 = pl.multiple_of((1 - q % 2) * 128, 128)

    def whole_rows(i, _):
        out_ref[i, pl.ds(a0, 128), :] = (gate[i, pl.ds(a0, 128), :] * projected(i, 12)).astype(BF16)
        return 0

    def half_rows(p, _):
        both = projected(p, 6)
        for e in range(2):
            out_ref[2 * p + e, pl.ds(b0, 64), :] = (
                gate[2 * p + e, pl.ds(b0, 64), :] * both[e * 64 : (e + 1) * 64]
            ).astype(BF16)
        return 0

    pltpu.make_async_copy(in_a, in_a, a_sem).wait()
    unpack(in_a.reshape(NC * 12, 128), 6)
    lax.fori_loop(0, 12, whole_rows, 0, unroll=UNROLL)
    pltpu.make_async_copy(in_b, in_b, b_sem).wait()
    unpack(in_b.reshape(NC * 6, 128), 3)
    lax.fori_loop(0, 6, half_rows, 0, unroll=UNROLL)
    for sent in (msg_r, msg_l, in_a, in_b):
        sent = sent.at[pl.ds(0, NC - 1)]
        pltpu.make_async_copy(sent, sent, send_sem).wait()
    pltpu.make_async_copy(r_own, r_own, swap_send).wait()


def local(*args):
    hbm = pl.BlockSpec(memory_space=pltpu.HBM)
    vmem = pl.BlockSpec(memory_space=pltpu.VMEM)
    dma = pltpu.SemaphoreType.DMA
    return pl.pallas_call(
        kernel,
        out_shape=jax.ShapeDtypeStruct((ROWS, COLS, WIDTH), BF16),
        in_specs=[hbm] * 8,
        out_specs=vmem,
        scratch_shapes=[
            pltpu.VMEM((ROWS, COLS, WIDTH), BF16),
            pltpu.SMEM((12, 12), jnp.int32),
            pltpu.VMEM((6, WIDTH, WIDTH), BF16),
            pltpu.VMEM((4 * WIDTH, WIDTH), BF16),
            pltpu.VMEM((ROWS, COLS, WIDTH), BF16),
            pltpu.VMEM((6, 256, WIDTH), BF16),
            pltpu.VMEM((ROWS, COLS, WIDTH), F32),
            pltpu.VMEM((NC * 24, 128), F32),
            pltpu.VMEM((NC, 2, 3, 4, 128), BF16),
            pltpu.VMEM((NC, 3, 4, 128), BF16),
            pltpu.VMEM((2, NX, NS, 3, 4, 128), BF16),
            pltpu.VMEM((2, NX, NS, 2, 3, 4, 128), BF16),
            pltpu.VMEM((2, 768, 128), BF16),
            pltpu.VMEM((NX, NS, 3, 4, 128), BF16),
            pltpu.VMEM((2, 96, 128), F32),
            pltpu.VMEM((NX, NS, 6, 2, 128), BF16),
            pltpu.VMEM((NX, NS, 3, 2, 128), BF16),
            pltpu.VMEM((NC, 6, 2, 128), BF16),
            pltpu.VMEM((NC, 3, 2, 128), BF16),
            dma((4,)), dma, dma((NX,)), dma((4,)), dma, dma, dma, dma, dma,
            pltpu.SemaphoreType.REGULAR, pltpu.SemaphoreType.REGULAR,
        ],
        compiler_params=pltpu.CompilerParams(
            collective_id=0, has_side_effects=True, vmem_limit_bytes=40 * 2**20
        ),
    )(*(pltpu.with_memory_space_constraint(a, pltpu.HBM) for a in args))


def solution(mesh):
    return jax.shard_map(
        local,
        mesh=mesh,
        in_specs=(P("row", "col", None), P(), P(), P(), P(), P(), P(), P()),
        out_specs=P("row", "col", None),
        check_vma=False,
    )
```

```python
import functools

import jax
import jax.numpy as jnp
from jax import lax
from jax.experimental import pallas as pl
from jax.experimental.pallas import tpu as pltpu
from jax.sharding import PartitionSpec as P

MESH = pl.DeviceIdType.MESH
NX, NY, NZ, NS, NC = 4, 4, 8, 32, 128
ROWS, COLS, WIDTH = 12, 192, 128
F32, BF16 = jnp.float32, jnp.bfloat16
UNROLL, UNROLL_PREP = 3, 3


def unit_norm(values, axis):
    mean = jnp.mean(values, axis=axis, keepdims=True)
    centred = values - mean
    spread = jnp.mean(centred * centred, axis=axis, keepdims=True)
    return centred * lax.rsqrt(spread + 1e-05)


def kernel(
    x_hbm, tm_hbm, wlg_hbm, wl_hbm, wrg_hbm, wr_hbm, wog_hbm, wo_hbm, out_ref,
    x_ref, tm_ref, w_in, wt, normed, masked, gate, stage, msg_r, msg_b, msg_l, r_own, r_all, r_mix, l_own,
    t_odd, t_a, t_b, in_a, in_b,
    load_sem, send_sem, r_sem, l_sem, a_sem, b_sem, swap_sem, swap_send, keep_sem, line_y, line_x,
):
    row, q = lax.axis_index("row"), lax.axis_index("col")
    core, y, z = row % 2, (row // 2) % NY, row // (2 * NY)
    s = row // 2
    chip = s * NX + q
    other = ((s * 2) + 1 - core, q)

    weights = (wlg_hbm, wl_hbm, wrg_hbm, wr_hbm, wog_hbm, wo_hbm)
    for n, w in enumerate(weights):
        pltpu.make_async_copy(w, w_in.at[n], load_sem.at[0]).start()
    load_mask = pltpu.make_async_copy(tm_hbm, tm_ref, load_sem.at[1])
    load_mask.start()
    load_x = [
        pltpu.make_async_copy(x_hbm.at[pl.ds(6 * n, 6)], x_ref.at[pl.ds(6 * n, 6)], load_sem.at[2 + n])
        for n in range(2)
    ]
    for load in load_x:
        load.start()

    xs = [(q + d) % NX for d in range(NX)]
    ys = [(y + d) % NY for d in range(NY)]

    def at(zz, yy, xx):
        return ((zz * NY + yy) * 2 + core, xx)

    x_line = [at(z, y, (q + d) % NX) for d in range(1, NX)]
    y_line = [at(z, (y + d) % NY, q) for d in range(1, NY)]
    z_line = [at((z + d) % NZ, y, q) for d in (4, 3, 5, 2, 6, 1, 7)]
    barrier = pltpu.get_barrier_semaphore()
    for peer in [*z_line, *y_line, *x_line, other]:
        pl.semaphore_signal(barrier, inc=1, device_id=peer, device_id_type=MESH)

    pltpu.make_async_copy(w_in, w_in, load_sem.at[0]).wait()
    for n in range(4):
        wt[n * WIDTH : (n + 1) * WIDTH, :] = w_in[n].astype(F32).T.astype(BF16)
    low = lax.broadcasted_iota(jnp.int32, (WIDTH, 128), 1) < 64
    odd_q = q % 2 == 1
    load_mask.wait()

    def project(n, values):
        return lax.dot_general(
            wt[n * WIDTH : (n + 1) * WIDTH, :], values, (((1,), (1,)), ((), ())),
            preferred_element_type=F32,
        )

    def store(n, rows):
        stage[pl.ds(n, NC, stride=12), :] = rows

    def right_rows(p, _):
        parts = {}
        for e in range(2):
            i = 2 * p + e
            n = unit_norm(x_ref[i].astype(F32), 1)
            normed[i] = n.astype(BF16)
            tile = (row * ROWS + i) // 64
            for t in range(3):
                m = tm_ref[tile, q * 3 + t].astype(F32)
                parts[e, t] = (n[t * 64 : (t + 1) * 64] * m).astype(BF16)
        firsts = jnp.concatenate([parts[0, 0], parts[0, 1], parts[1, 0], parts[1, 1]], axis=0)
        masked[p, 0:256, :] = firsts
        masked[p, 256:384, :] = jnp.concatenate([parts[0, 2], parts[1, 2]], axis=0)
        right = jax.nn.sigmoid(project(2, firsts)) * project(3, firsts)
        for e in range(2):
            store(2 * p + e, right[:, e * 128 : (e + 1) * 128])
        return 0

    def shared_rows(p, _):
        lasts = masked[p, 256:384, :]
        right = jax.nn.sigmoid(project(2, lasts)) * project(3, lasts)
        left = jax.nn.sigmoid(project(0, lasts)) * project(1, lasts)
        first, second = jnp.where(odd_q, right, left), jnp.where(odd_q, left, right)
        store(2 * p, jnp.where(low, first, pltpu.roll(second, 64, 1)))
        store(2 * p + 1, jnp.where(low, pltpu.roll(first, 64, 1), second))
        return 0

    def left_rows(p, _):
        firsts = masked[p, 0:256, :]
        left = jax.nn.sigmoid(project(0, firsts)) * project(1, firsts)
        for e in range(2):
            store(2 * p + e, left[:, e * 128 : (e + 1) * 128])
        return 0

    def pack(message):
        target = message.reshape(NC * 12, 128)

        def some(n, _):
            rows = pl.ds(pl.multiple_of(n * 256, 256), 256)
            target[rows, :] = stage[rows, :].astype(BF16)
            return 0

        lax.fori_loop(0, 6, some, 0)

    def send_r(kind, dx, k, dys):
        zz, xx = (z + 4 + ((k + 1) // 2) * (1 - 2 * (k % 2))) % NZ, (q + dx) % NX
        for dy in dys:
            ss = zz * NY + ys[dy]
            pltpu.make_async_remote_copy(
                (msg_r, msg_b)[kind].at[ss * NX + xx], r_own.at[kind, q, s],
                send_sem, r_sem.at[4 * kind + dx],
                device_id=(ss * 2 + core, xx), device_id_type=MESH,
            ).start()
        return 0

    load_x[0].wait()
    lax.fori_loop(0, 3, right_rows, 0, unroll=UNROLL_PREP)
    load_x[1].wait()
    lax.fori_loop(3, 6, right_rows, 0, unroll=UNROLL_PREP)
    pack(msg_r)
    pl.semaphore_wait(barrier, 1 + 3 + 3 + 7)
    for peer in y_line:
        pl.semaphore_signal(line_y, inc=1, device_id=peer, device_id_type=MESH)
    pltpu.make_async_copy(msg_r.at[chip], r_own.at[0, q, s], r_sem.at[0]).start()
    lax.fori_loop(0, 7, lambda k, _: send_r(0, 0, k, (0,)), 0)
    pl.semaphore_wait(line_y, 3)
    for peer in x_line:
        pl.semaphore_signal(line_x, inc=1, device_id=peer, device_id_type=MESH)
    lax.fori_loop(0, 8, lambda k, _: send_r(0, 0, k, (1, 2, 3)), 0)
    pl.semaphore_wait(line_x, 3)
    lax.fori_loop(8, 32, lambda n, _: send_r(0, n // 8, n % 8, range(4)), 0)

    lax.fori_loop(0, 6, shared_rows, 0, unroll=UNROLL_PREP)
    pack(msg_b)
    pltpu.make_async_copy(msg_b.at[chip], r_own.at[1, q, s], r_sem.at[4]).start()
    lax.fori_loop(0, 7, lambda k, _: send_r(1, 0, k, range(4)), 0)
    send_r(1, 0, 7, (1, 2, 3))
    lax.fori_loop(8, 32, lambda n, _: send_r(1, n // 8, n % 8, range(4)), 0)

    lax.fori_loop(0, 6, left_rows, 0, unroll=UNROLL_PREP)
    pack(msg_l)

    def offset(g, e):
        return 4 - g if e == 0 else 4 + g + 4 * ((3 - g) // 3)

    def to_all(send):
        def eight(n, skip):
            g = n // 4
            yy = (y + n) % NY
            for e in range(2):
                ss = ((z + offset(g, e)) % NZ) * NY + yy
                for d in range(NX):
                    if (e, d) != skip:
                        send(g, ss, xs[d])
            return 0

        eight(0, (1, 0))
        lax.fori_loop(1, 16, lambda n, _: eight(n, None), 0)

    def send_l(g, ss, xx):
        pltpu.make_async_remote_copy(
            msg_l.at[ss * NX + xx], l_own.at[q, s], send_sem, l_sem.at[g],
            device_id=(ss * 2 + core, xx), device_id_type=MESH,
        ).start()

    pltpu.make_async_copy(msg_l.at[chip], l_own.at[q, s], l_sem.at[0]).start()
    to_all(send_l)

    def gates(i, _):
        gate[i] = jax.nn.sigmoid(jnp.dot(normed[i], w_in[4], preferred_element_type=F32))
        return 0

    lax.fori_loop(0, ROWS, gates, 0)

    def swap(n, _):
        kind, xx = n // NX, (q + NX - n % NX) % NX
        block, mine = r_own.at[kind, xx], r_all.at[kind, xx, :, core]
        pltpu.make_async_copy(block, block, r_sem.at[n]).wait()
        pltpu.make_async_remote_copy(
            block, mine, swap_send, swap_sem, device_id=other, device_id_type=MESH
        ).start()
        pltpu.make_async_copy(block, mine, keep_sem).start()
        return 0

    lax.fori_loop(0, 2 * NX, swap, 0)
    pltpu.make_async_copy(r_own, r_own, keep_sem).wait()
    pltpu.make_async_copy(r_own, r_own, swap_sem).wait()

    ra = r_all.reshape(2 * NX * 768, 128)
    rb = r_own.reshape(2 * NX * 384, 128)
    la = l_own.reshape(NX * 384, 128)
    whole = t_a.reshape(NX * 384, 128)
    halves = t_b.reshape(NX * 192, 128)

    def block(ref, n, size):
        return ref[n * size : (n + 1) * size, :]

    for n, x in enumerate((0, 2)):
        r_mix[n] = jnp.concatenate(
            [block(ra, NX + x, 768)[:, 64:], block(ra, NX + x + 1, 768)[:, :64]], axis=1
        )
    lane_b = lax.broadcasted_iota(jnp.int32, (48, 128), 1) < 64

    def rows_of(g, _):
        places = [(z + NZ - offset(g, e)) % NZ for e in range(2)]
        arrived = msg_l.at[pl.ds(0, 32)]
        pltpu.make_async_copy(arrived, arrived, l_sem.at[g]).wait()

        def part(ref, n):
            return jnp.concatenate(
                [ref[pl.ds(pl.multiple_of(n * 384 + zz * 48, 48), 48), :] for zz in places], axis=0
            )

        lhs = [part(la, x) for x in range(NX)]
        for x in (0, 2):
            lhs.append(
                jnp.concatenate([part(rb, NX + x)[:, :64], part(rb, NX + x + 1)[:, 64:]], axis=1)
            )
        rhs = [block(ra, x, 768) for x in range(NX)] + [r_mix[0], r_mix[1]]
        triangle = lax.dot_general(
            jnp.concatenate(lhs, axis=1), jnp.concatenate(rhs, axis=1), (((1,), (1,)), ((), ())),
            preferred_element_type=F32,
        )
        for e, zz in enumerate(places):
            for x, tile in enumerate((0, 2, 3, 5)):
                whole[pl.ds(pl.multiple_of(x * 384 + zz * 48, 48), 48), :] = triangle[
                    e * 48 : (e + 1) * 48, tile * 128 : (tile + 1) * 128
                ].astype(BF16)

        def back(dy, _):
            for e, zz in enumerate(places):
                ss = zz * NY + (y + dy) % NY
                for d in range(NX):

                    def send(ss=ss, xx=xs[d]):
                        pltpu.make_async_remote_copy(
                            t_a.at[xx, ss], in_a.at[chip], send_sem, a_sem,
                            device_id=(ss * 2 + core, xx), device_id_type=MESH,
                        ).start()

                    if (e, d) == (1, 0):
                        pl.when((g != 0) | (dy != 0))(send)
                    else:
                        send()
            return 0

        lax.fori_loop(0, NY, back, 0)
        for n, tile in enumerate((1, 4)):
            t_odd[n] = triangle[:, tile * 128 : (tile + 1) * 128]
            even, odd = t_odd[n, pl.ds(0, 48, stride=2), :], t_odd[n, pl.ds(1, 48, stride=2), :]
            both = (
                jnp.where(lane_b, even, pltpu.roll(odd, 64, 1)),
                jnp.where(lane_b, pltpu.roll(even, 64, 1), odd),
            )
            for e, zz in enumerate(places):
                for h in range(2):
                    halves[pl.ds(pl.multiple_of((2 * n + h) * 192 + zz * 24, 8), 24), :] = both[h][
                        e * 24 : (e + 1) * 24
                    ].astype(BF16)
        return 0

    lax.fori_loop(0, 4, rows_of, 0)
    pltpu.make_async_copy(t_a.at[q, s], in_a.at[chip], a_sem).start()
    pltpu.make_async_copy(t_b.at[q, s], in_b.at[chip], b_sem).start()

    def send_b(g, ss, xx):
        pltpu.make_async_remote_copy(
            t_b.at[xx, ss], in_b.at[chip], send_sem, b_sem,
            device_id=(ss * 2 + core, xx), device_id_type=MESH,
        ).start()

    to_all(send_b)

    def unpack(source, steps):
        def some(n, _):
            rows = pl.ds(pl.multiple_of(n * 256, 256), 256)
            stage[rows, :] = source[rows, :].astype(F32)
            return 0

        lax.fori_loop(0, steps, some, 0)

    def projected(g, stride):
        scaled = unit_norm(stage[pl.ds(g, NC, stride=stride), :], 0)
        return jnp.dot(scaled.T.astype(BF16), w_in[5], preferred_element_type=F32)

    a0 = pl.multiple_of((q % 2) * 64, 64)
    b0 = pl.multiple_of((1 - q % 2) * 128, 128)

    def whole_rows(i, _):
        out_ref[i, pl.ds(a0, 128), :] = (gate[i, pl.ds(a0, 128), :] * projected(i, 12)).astype(BF16)
        return 0

    def half_rows(p, _):
        both = projected(p, 6)
        for e in range(2):
            out_ref[2 * p + e, pl.ds(b0, 64), :] = (
                gate[2 * p + e, pl.ds(b0, 64), :] * both[e * 64 : (e + 1) * 64]
            ).astype(BF16)
        return 0

    pltpu.make_async_copy(in_a, in_a, a_sem).wait()
    unpack(in_a.reshape(NC * 12, 128), 6)
    lax.fori_loop(0, 12, whole_rows, 0, unroll=UNROLL)
    pltpu.make_async_copy(in_b, in_b, b_sem).wait()
    unpack(in_b.reshape(NC * 6, 128), 3)
    lax.fori_loop(0, 6, half_rows, 0, unroll=UNROLL)
    for sent in (msg_r, msg_b, msg_l, in_a, in_b):
        sent = sent.at[pl.ds(0, NC - 1)]
        pltpu.make_async_copy(sent, sent, send_sem).wait()
    pltpu.make_async_copy(r_own, r_own, swap_send).wait()


def local(*args):
    hbm = pl.BlockSpec(memory_space=pltpu.HBM)
    vmem = pl.BlockSpec(memory_space=pltpu.VMEM)
    dma = pltpu.SemaphoreType.DMA
    return pl.pallas_call(
        kernel,
        out_shape=jax.ShapeDtypeStruct((ROWS, COLS, WIDTH), BF16),
        in_specs=[hbm] * 8,
        out_specs=vmem,
        scratch_shapes=[
            pltpu.VMEM((ROWS, COLS, WIDTH), BF16),
            pltpu.SMEM((12, 12), jnp.int32),
            pltpu.VMEM((6, WIDTH, WIDTH), BF16),
            pltpu.VMEM((4 * WIDTH, WIDTH), BF16),
            pltpu.VMEM((ROWS, COLS, WIDTH), BF16),
            pltpu.VMEM((6, 384, WIDTH), BF16),
            pltpu.VMEM((ROWS, COLS, WIDTH), F32),
            pltpu.VMEM((NC * 12, 128), F32),
            pltpu.VMEM((NC, 3, 4, 128), BF16),
            pltpu.VMEM((NC, 3, 4, 128), BF16),
            pltpu.VMEM((NC, 3, 4, 128), BF16),
            pltpu.VMEM((2, NX, NS, 3, 4, 128), BF16),
            pltpu.VMEM((2, NX, NS, 2, 3, 4, 128), BF16),
            pltpu.VMEM((2, 768, 128), BF16),
            pltpu.VMEM((NX, NS, 3, 4, 128), BF16),
            pltpu.VMEM((2, 96, 128), F32),
            pltpu.VMEM((NX, NS, 6, 2, 128), BF16),
            pltpu.VMEM((NX, NS, 3, 2, 128), BF16),
            pltpu.VMEM((NC, 6, 2, 128), BF16),
            pltpu.VMEM((NC, 3, 2, 128), BF16),
            dma((4,)), dma, dma((2 * NX,)), dma((4,)), dma, dma, dma, dma, dma,
            pltpu.SemaphoreType.REGULAR, pltpu.SemaphoreType.REGULAR,
        ],
        compiler_params=pltpu.CompilerParams(
            collective_id=0, has_side_effects=True, vmem_limit_bytes=40 * 2**20
        ),
    )(*(pltpu.with_memory_space_constraint(a, pltpu.HBM) for a in args))


def solution(mesh):
    return jax.shard_map(
        local,
        mesh=mesh,
        in_specs=(P("row", "col", None), P(), P(), P(), P(), P(), P(), P()),
        out_specs=P("row", "col", None),
        check_vma=False,
    )
```

```python
import functools

import jax
import jax.numpy as jnp
from jax import lax
from jax.experimental import pallas as pl
from jax.experimental.pallas import tpu as pltpu
from jax.sharding import PartitionSpec as P

MESH = pl.DeviceIdType.MESH
NX, NY, NZ, NS, NC = 4, 4, 8, 32, 128
ROWS, COLS, WIDTH = 12, 192, 128
F32, BF16 = jnp.float32, jnp.bfloat16
UNROLL, UNROLL_PREP = 6, 3


def unit_norm(values, axis):
    mean = jnp.mean(values, axis=axis, keepdims=True)
    centred = values - mean
    spread = jnp.mean(centred * centred, axis=axis, keepdims=True)
    return centred * lax.rsqrt(spread + 1e-05)


def kernel(
    x_hbm, tm_hbm, wlg_hbm, wl_hbm, wrg_hbm, wr_hbm, wog_hbm, wo_hbm, out_ref,
    x_ref, tm_ref, w_in, wt, normed, masked, gate, stage, msg_r, msg_b, msg_l, r_own, r_all, r_mix, l_own,
    t_odd, t_a, t_b, in_a, in_b,
    load_sem, send_sem, r_sem, l_sem, a_sem, b_sem, swap_sem, swap_send, keep_sem, line_y, line_x,
):
    row, q = lax.axis_index("row"), lax.axis_index("col")
    core, y, z = row % 2, (row // 2) % NY, row // (2 * NY)
    s = row // 2
    chip = s * NX + q
    other = ((s * 2) + 1 - core, q)

    weights = (wlg_hbm, wl_hbm, wrg_hbm, wr_hbm, wog_hbm, wo_hbm)
    for n, w in enumerate(weights):
        pltpu.make_async_copy(w, w_in.at[n], load_sem.at[0]).start()
    load_mask = pltpu.make_async_copy(tm_hbm, tm_ref, load_sem.at[1])
    load_mask.start()
    load_x = [
        pltpu.make_async_copy(x_hbm.at[pl.ds(6 * n, 6)], x_ref.at[pl.ds(6 * n, 6)], load_sem.at[2 + n])
        for n in range(2)
    ]
    for load in load_x:
        load.start()

    xs = [(q + d) % NX for d in range(NX)]
    ys = [(y + d) % NY for d in range(NY)]

    def at(zz, yy, xx):
        return ((zz * NY + yy) * 2 + core, xx)

    x_line = [at(z, y, (q + d) % NX) for d in range(1, NX)]
    y_line = [at(z, (y + d) % NY, q) for d in range(1, NY)]
    z_line = [at((z + d) % NZ, y, q) for d in (4, 3, 5, 2, 6, 1, 7)]
    barrier = pltpu.get_barrier_semaphore()
    for peer in [*z_line, *y_line, *x_line, other]:
        pl.semaphore_signal(barrier, inc=1, device_id=peer, device_id_type=MESH)

    pltpu.make_async_copy(w_in, w_in, load_sem.at[0]).wait()
    for n in range(4):
        wt[n * WIDTH : (n + 1) * WIDTH, :] = w_in[n].astype(F32).T.astype(BF16)
    low = lax.broadcasted_iota(jnp.int32, (WIDTH, 128), 1) < 64
    odd_q = q % 2 == 1
    load_mask.wait()

    def project(n, values):
        return lax.dot_general(
            wt[n * WIDTH : (n + 1) * WIDTH, :], values, (((1,), (1,)), ((), ())),
            preferred_element_type=F32,
        )

    def store(n, rows):
        stage[pl.ds(n, NC, stride=12), :] = rows

    def right_rows(p, _):
        parts = {}
        for e in range(2):
            i = 2 * p + e
            n = unit_norm(x_ref[i].astype(F32), 1)
            normed[i] = n.astype(BF16)
            tile = (row * ROWS + i) // 64
            for t in range(3):
                m = tm_ref[tile, q * 3 + t].astype(F32)
                parts[e, t] = (n[t * 64 : (t + 1) * 64] * m).astype(BF16)
        firsts = jnp.concatenate([parts[0, 0], parts[0, 1], parts[1, 0], parts[1, 1]], axis=0)
        masked[p, 0:256, :] = firsts
        masked[p, 256:384, :] = jnp.concatenate([parts[0, 2], parts[1, 2]], axis=0)
        right = jax.nn.sigmoid(project(2, firsts)) * project(3, firsts)
        for e in range(2):
            store(2 * p + e, right[:, e * 128 : (e + 1) * 128])
        return 0

    def shared_rows(p, _):
        lasts = masked[p, 256:384, :]
        right = jax.nn.sigmoid(project(2, lasts)) * project(3, lasts)
        left = jax.nn.sigmoid(project(0, lasts)) * project(1, lasts)
        first, second = jnp.where(odd_q, right, left), jnp.where(odd_q, left, right)
        store(2 * p, jnp.where(low, first, pltpu.roll(second, 64, 1)))
        store(2 * p + 1, jnp.where(low, pltpu.roll(first, 64, 1), second))
        return 0

    def left_rows(p, _):
        firsts = masked[p, 0:256, :]
        left = jax.nn.sigmoid(project(0, firsts)) * project(1, firsts)
        for e in range(2):
            store(2 * p + e, left[:, e * 128 : (e + 1) * 128])
        return 0

    def pack(message):
        target = message.reshape(NC * 12, 128)

        def some(n, _):
            rows = pl.ds(pl.multiple_of(n * 256, 256), 256)
            target[rows, :] = stage[rows, :].astype(BF16)
            return 0

        lax.fori_loop(0, 6, some, 0)

    def send_r(kind, dx, k, dys):
        zz, xx = (z + 4 + ((k + 1) // 2) * (1 - 2 * (k % 2))) % NZ, (q + dx) % NX
        for dy in dys:
            ss = zz * NY + ys[dy]
            pltpu.make_async_remote_copy(
                (msg_r, msg_b)[kind].at[ss * NX + xx], r_own.at[kind, q, s],
                send_sem, r_sem.at[4 * kind + dx],
                device_id=(ss * 2 + core, xx), device_id_type=MESH,
            ).start()
        return 0

    load_x[0].wait()
    lax.fori_loop(0, 3, right_rows, 0, unroll=UNROLL_PREP)
    load_x[1].wait()
    lax.fori_loop(3, 6, right_rows, 0, unroll=UNROLL_PREP)
    pack(msg_r)
    pl.semaphore_wait(barrier, 1 + 3 + 3 + 7)
    for peer in y_line:
        pl.semaphore_signal(line_y, inc=1, device_id=peer, device_id_type=MESH)
    pltpu.make_async_copy(msg_r.at[chip], r_own.at[0, q, s], r_sem.at[0]).start()
    lax.fori_loop(0, 7, lambda k, _: send_r(0, 0, k, (0,)), 0)
    pl.semaphore_wait(line_y, 3)
    for peer in x_line:
        pl.semaphore_signal(line_x, inc=1, device_id=peer, device_id_type=MESH)
    lax.fori_loop(0, 8, lambda k, _: send_r(0, 0, k, (1, 2, 3)), 0)
    pl.semaphore_wait(line_x, 3)
    lax.fori_loop(8, 32, lambda n, _: send_r(0, n // 8, n % 8, range(4)), 0)

    lax.fori_loop(0, 6, shared_rows, 0, unroll=UNROLL_PREP)
    pack(msg_b)
    pltpu.make_async_copy(msg_b.at[chip], r_own.at[1, q, s], r_sem.at[4]).start()
    lax.fori_loop(0, 7, lambda k, _: send_r(1, 0, k, range(4)), 0)
    send_r(1, 0, 7, (1, 2, 3))
    lax.fori_loop(8, 32, lambda n, _: send_r(1, n // 8, n % 8, range(4)), 0)

    lax.fori_loop(0, 6, left_rows, 0, unroll=UNROLL_PREP)
    pack(msg_l)

    def offset(g, e):
        return 4 - g if e == 0 else 4 + g + 4 * ((3 - g) // 3)

    def to_all(send):
        def eight(n, skip):
            g = n // 4
            yy = (y + n) % NY
            for e in range(2):
                ss = ((z + offset(g, e)) % NZ) * NY + yy
                for d in range(NX):
                    if (e, d) != skip:
                        send(g, ss, xs[d])
            return 0

        eight(0, (1, 0))
        lax.fori_loop(1, 16, lambda n, _: eight(n, None), 0)

    def send_l(g, ss, xx):
        pltpu.make_async_remote_copy(
            msg_l.at[ss * NX + xx], l_own.at[q, s], send_sem, l_sem.at[g],
            device_id=(ss * 2 + core, xx), device_id_type=MESH,
        ).start()

    pltpu.make_async_copy(msg_l.at[chip], l_own.at[q, s], l_sem.at[0]).start()
    to_all(send_l)

    def gates(i, _):
        gate[i] = jax.nn.sigmoid(jnp.dot(normed[i], w_in[4], preferred_element_type=F32))
        return 0

    lax.fori_loop(0, ROWS, gates, 0)

    def swap(n, _):
        kind, xx = n // NX, (q + NX - n % NX) % NX
        block, mine = r_own.at[kind, xx], r_all.at[kind, xx, :, core]
        pltpu.make_async_copy(block, block, r_sem.at[n]).wait()
        pltpu.make_async_remote_copy(
            block, mine, swap_send, swap_sem, device_id=other, device_id_type=MESH
        ).start()
        pltpu.make_async_copy(block, mine, keep_sem).start()
        return 0

    lax.fori_loop(0, 2 * NX, swap, 0)
    pltpu.make_async_copy(r_own, r_own, keep_sem).wait()
    pltpu.make_async_copy(r_own, r_own, swap_sem).wait()

    ra = r_all.reshape(2 * NX * 768, 128)
    rb = r_own.reshape(2 * NX * 384, 128)
    la = l_own.reshape(NX * 384, 128)
    whole = t_a.reshape(NX * 384, 128)
    halves = t_b.reshape(NX * 192, 128)

    def block(ref, n, size):
        return ref[n * size : (n + 1) * size, :]

    for n, x in enumerate((0, 2)):
        r_mix[n] = jnp.concatenate(
            [block(ra, NX + x, 768)[:, 64:], block(ra, NX + x + 1, 768)[:, :64]], axis=1
        )
    lane_b = lax.broadcasted_iota(jnp.int32, (48, 128), 1) < 64

    def rows_of(g, _):
        places = [(z + NZ - offset(g, e)) % NZ for e in range(2)]
        arrived = msg_l.at[pl.ds(0, 32)]
        pltpu.make_async_copy(arrived, arrived, l_sem.at[g]).wait()

        def part(ref, n):
            return jnp.concatenate(
                [ref[pl.ds(pl.multiple_of(n * 384 + zz * 48, 48), 48), :] for zz in places], axis=0
            )

        lhs = [part(la, x) for x in range(NX)]
        for x in (0, 2):
            lhs.append(
                jnp.concatenate([part(rb, NX + x)[:, :64], part(rb, NX + x + 1)[:, 64:]], axis=1)
            )
        rhs = [block(ra, x, 768) for x in range(NX)] + [r_mix[0], r_mix[1]]
        triangle = lax.dot_general(
            jnp.concatenate(lhs, axis=1), jnp.concatenate(rhs, axis=1), (((1,), (1,)), ((), ())),
            preferred_element_type=F32,
        )
        for e, zz in enumerate(places):
            for x, tile in enumerate((0, 2, 3, 5)):
                whole[pl.ds(pl.multiple_of(x * 384 + zz * 48, 48), 48), :] = triangle[
                    e * 48 : (e + 1) * 48, tile * 128 : (tile + 1) * 128
                ].astype(BF16)

        def back(dy, _):
            for e, zz in enumerate(places):
                ss = zz * NY + (y + dy) % NY
                for d in range(NX):

                    def send(ss=ss, xx=xs[d]):
                        pltpu.make_async_remote_copy(
                            t_a.at[xx, ss], in_a.at[chip], send_sem, a_sem,
                            device_id=(ss * 2 + core, xx), device_id_type=MESH,
                        ).start()

                    if (e, d) == (1, 0):
                        pl.when((g != 0) | (dy != 0))(send)
                    else:
                        send()
            return 0

        lax.fori_loop(0, NY, back, 0)
        for n, tile in enumerate((1, 4)):
            t_odd[n] = triangle[:, tile * 128 : (tile + 1) * 128]
            even, odd = t_odd[n, pl.ds(0, 48, stride=2), :], t_odd[n, pl.ds(1, 48, stride=2), :]
            both = (
                jnp.where(lane_b, even, pltpu.roll(odd, 64, 1)),
                jnp.where(lane_b, pltpu.roll(even, 64, 1), odd),
            )
            for e, zz in enumerate(places):
                for h in range(2):
                    halves[pl.ds(pl.multiple_of((2 * n + h) * 192 + zz * 24, 8), 24), :] = both[h][
                        e * 24 : (e + 1) * 24
                    ].astype(BF16)
        return 0

    lax.fori_loop(0, 4, rows_of, 0)
    pltpu.make_async_copy(t_a.at[q, s], in_a.at[chip], a_sem).start()
    pltpu.make_async_copy(t_b.at[q, s], in_b.at[chip], b_sem).start()

    def send_b(g, ss, xx):
        pltpu.make_async_remote_copy(
            t_b.at[xx, ss], in_b.at[chip], send_sem, b_sem,
            device_id=(ss * 2 + core, xx), device_id_type=MESH,
        ).start()

    to_all(send_b)

    def unpack(source, steps):
        def some(n, _):
            rows = pl.ds(pl.multiple_of(n * 256, 256), 256)
            stage[rows, :] = source[rows, :].astype(F32)
            return 0

        lax.fori_loop(0, steps, some, 0)

    def projected(g, stride):
        scaled = unit_norm(stage[pl.ds(g, NC, stride=stride), :], 0)
        return lax.dot_general(
            scaled.astype(BF16), w_in[5], (((0,), (0,)), ((), ())), preferred_element_type=F32
        )

    a0 = pl.multiple_of((q % 2) * 64, 64)
    b0 = pl.multiple_of((1 - q % 2) * 128, 128)

    def whole_rows(i, _):
        out_ref[i, pl.ds(a0, 128), :] = (gate[i, pl.ds(a0, 128), :] * projected(i, 12)).astype(BF16)
        return 0

    def half_rows(p, _):
        both = projected(p, 6)
        for e in range(2):
            out_ref[2 * p + e, pl.ds(b0, 64), :] = (
                gate[2 * p + e, pl.ds(b0, 64), :] * both[e * 64 : (e + 1) * 64]
            ).astype(BF16)
        return 0

    pltpu.make_async_copy(in_a, in_a, a_sem).wait()
    unpack(in_a.reshape(NC * 12, 128), 6)
    lax.fori_loop(0, 12, whole_rows, 0, unroll=UNROLL)
    pltpu.make_async_copy(in_b, in_b, b_sem).wait()
    unpack(in_b.reshape(NC * 6, 128), 3)
    lax.fori_loop(0, 6, half_rows, 0, unroll=UNROLL)
    for sent in (msg_r, msg_b, msg_l, in_a, in_b):
        sent = sent.at[pl.ds(0, NC - 1)]
        pltpu.make_async_copy(sent, sent, send_sem).wait()
    pltpu.make_async_copy(r_own, r_own, swap_send).wait()


def local(*args):
    hbm = pl.BlockSpec(memory_space=pltpu.HBM)
    vmem = pl.BlockSpec(memory_space=pltpu.VMEM)
    dma = pltpu.SemaphoreType.DMA
    return pl.pallas_call(
        kernel,
        out_shape=jax.ShapeDtypeStruct((ROWS, COLS, WIDTH), BF16),
        in_specs=[hbm] * 8,
        out_specs=vmem,
        scratch_shapes=[
            pltpu.VMEM((ROWS, COLS, WIDTH), BF16),
            pltpu.SMEM((12, 12), jnp.int32),
            pltpu.VMEM((6, WIDTH, WIDTH), BF16),
            pltpu.VMEM((4 * WIDTH, WIDTH), BF16),
            pltpu.VMEM((ROWS, COLS, WIDTH), BF16),
            pltpu.VMEM((6, 384, WIDTH), BF16),
            pltpu.VMEM((ROWS, COLS, WIDTH), F32),
            pltpu.VMEM((NC * 12, 128), F32),
            pltpu.VMEM((NC, 3, 4, 128), BF16),
            pltpu.VMEM((NC, 3, 4, 128), BF16),
            pltpu.VMEM((NC, 3, 4, 128), BF16),
            pltpu.VMEM((2, NX, NS, 3, 4, 128), BF16),
            pltpu.VMEM((2, NX, NS, 2, 3, 4, 128), BF16),
            pltpu.VMEM((2, 768, 128), BF16),
            pltpu.VMEM((NX, NS, 3, 4, 128), BF16),
            pltpu.VMEM((2, 96, 128), F32),
            pltpu.VMEM((NX, NS, 6, 2, 128), BF16),
            pltpu.VMEM((NX, NS, 3, 2, 128), BF16),
            pltpu.VMEM((NC, 6, 2, 128), BF16),
            pltpu.VMEM((NC, 3, 2, 128), BF16),
            dma((4,)), dma, dma((2 * NX,)), dma((4,)), dma, dma, dma, dma, dma,
            pltpu.SemaphoreType.REGULAR, pltpu.SemaphoreType.REGULAR,
        ],
        compiler_params=pltpu.CompilerParams(
            collective_id=0, has_side_effects=True, vmem_limit_bytes=40 * 2**20
        ),
    )(*(pltpu.with_memory_space_constraint(a, pltpu.HBM) for a in args))


def solution(mesh):
    return jax.shard_map(
        local,
        mesh=mesh,
        in_specs=(P("row", "col", None), P(), P(), P(), P(), P(), P(), P()),
        out_specs=P("row", "col", None),
        check_vma=False,
    )
```

```python
import functools

import jax
import jax.numpy as jnp
from jax import lax
from jax.experimental import pallas as pl
from jax.experimental.pallas import tpu as pltpu
from jax.sharding import PartitionSpec as P

MESH = pl.DeviceIdType.MESH
NX, NY, NZ, NS, NC = 4, 4, 8, 32, 128
ROWS, COLS, WIDTH = 12, 192, 128
F32, BF16 = jnp.float32, jnp.bfloat16
UNROLL, UNROLL_PREP = 6, 3


def unit_norm(values, axis):
    mean = jnp.mean(values, axis=axis, keepdims=True)
    centred = values - mean
    spread = jnp.mean(centred * centred, axis=axis, keepdims=True)
    return centred * lax.rsqrt(spread + 1e-05)


def kernel(
    x_hbm, tm_hbm, wlg_hbm, wl_hbm, wrg_hbm, wr_hbm, wog_hbm, wo_hbm, out_ref,
    x_ref, tm_ref, w_in, wt, normed, masked, gate, stage, msg_r, msg_b, msg_l, r_own, r_all, r_half, r_mix, l_own,
    t_odd, t_a, t_b, in_a, in_b,
    load_sem, send_sem, r_sem, l_sem, a_sem, b_sem, relay_sem, relay_send, swap_sem, swap_send, keep_sem,
    line_y, line_x,
):
    row, q = lax.axis_index("row"), lax.axis_index("col")
    core, y, z = row % 2, (row // 2) % NY, row // (2 * NY)
    s = row // 2
    channels = [s * NX + q, (((z + NZ - 1) % NZ) * NY + y) * NX + q]
    other = ((s * 2) + 1 - core, q)

    weights = (wlg_hbm, wl_hbm, wrg_hbm, wr_hbm, wog_hbm, wo_hbm)
    for n, w in enumerate(weights):
        pltpu.make_async_copy(w, w_in.at[n], load_sem.at[0]).start()
    load_mask = pltpu.make_async_copy(tm_hbm, tm_ref, load_sem.at[1])
    load_mask.start()
    load_x = [
        pltpu.make_async_copy(x_hbm.at[pl.ds(6 * n, 6)], x_ref.at[pl.ds(6 * n, 6)], load_sem.at[2 + n])
        for n in range(2)
    ]
    for load in load_x:
        load.start()

    xs = [(q + d) % NX for d in range(NX)]
    ys = [(y + d) % NY for d in range(NY)]

    def at(zz, yy, xx):
        return ((zz * NY + yy) * 2 + core, xx)

    x_line = [at(z, y, (q + d) % NX) for d in range(1, NX)]
    y_line = [at(z, (y + d) % NY, q) for d in range(1, NY)]
    z_line = [at((z + d) % NZ, y, q) for d in (4, 3, 5, 2, 6, 1, 7)]
    barrier = pltpu.get_barrier_semaphore()
    for peer in [*z_line, *y_line, *x_line, other]:
        pl.semaphore_signal(barrier, inc=1, device_id=peer, device_id_type=MESH)

    pltpu.make_async_copy(w_in, w_in, load_sem.at[0]).wait()
    for n in range(4):
        wt[n * WIDTH : (n + 1) * WIDTH, :] = w_in[n].astype(F32).T.astype(BF16)
    low = lax.broadcasted_iota(jnp.int32, (WIDTH, 128), 1) < 64
    odd_q = q % 2 == 1
    load_mask.wait()

    def project(n, values):
        return lax.dot_general(
            wt[n * WIDTH : (n + 1) * WIDTH, :], values, (((1,), (1,)), ((), ())),
            preferred_element_type=F32,
        )

    def store(n, rows):
        stage[pl.ds(n, NC, stride=12), :] = rows

    def right_rows(p, _):
        parts = {}
        for e in range(2):
            i = 2 * p + e
            n = unit_norm(x_ref[i].astype(F32), 1)
            normed[i] = n.astype(BF16)
            tile = (row * ROWS + i) // 64
            for t in range(3):
                m = tm_ref[tile, q * 3 + t].astype(F32)
                parts[e, t] = (n[t * 64 : (t + 1) * 64] * m).astype(BF16)
        firsts = jnp.concatenate([parts[0, 0], parts[0, 1], parts[1, 0], parts[1, 1]], axis=0)
        masked[p, 0:256, :] = firsts
        masked[p, 256:384, :] = jnp.concatenate([parts[0, 2], parts[1, 2]], axis=0)
        right = jax.nn.sigmoid(project(2, firsts)) * project(3, firsts)
        for e in range(2):
            store(2 * p + e, right[:, e * 128 : (e + 1) * 128])
        return 0

    def shared_rows(p, _):
        lasts = masked[p, 256:384, :]
        right = jax.nn.sigmoid(project(2, lasts)) * project(3, lasts)
        left = jax.nn.sigmoid(project(0, lasts)) * project(1, lasts)
        first, second = jnp.where(odd_q, right, left), jnp.where(odd_q, left, right)
        store(2 * p, jnp.where(low, first, pltpu.roll(second, 64, 1)))
        store(2 * p + 1, jnp.where(low, pltpu.roll(first, 64, 1), second))
        return 0

    def left_rows(p, _):
        firsts = masked[p, 0:256, :]
        left = jax.nn.sigmoid(project(0, firsts)) * project(1, firsts)
        for e in range(2):
            store(2 * p + e, left[:, e * 128 : (e + 1) * 128])
        return 0

    def pack(message):
        target = message.reshape(NC * 12, 128)

        def some(n, _):
            rows = pl.ds(pl.multiple_of(n * 256, 256), 256)
            target[rows, :] = stage[rows, :].astype(BF16)
            return 0

        lax.fori_loop(0, 6, some, 0)

    def ends(k):
        slot = k % 2
        zz = (z + NZ + (3 - k // 2) * (1 - 2 * slot)) % NZ
        return slot, zz, (zz + NZ - slot) % NZ

    def send_r(kind, k, dxs, dys):
        slot, zz, d = ends(k)
        for dy in dys:
            for dx in dxs:
                pltpu.make_async_remote_copy(
                    (msg_r, msg_b)[kind].at[(d * NY + ys[dy]) * NX + xs[dx]],
                    r_own.at[kind, slot, q, s], send_sem, r_sem.at[4 * kind + k // 2],
                    device_id=((zz * NY + ys[dy]) * 2 + core, xs[dx]), device_id_type=MESH,
                ).start()
        return 0

    def keep_r(kind):
        for slot in range(2):
            pltpu.make_async_copy(
                (msg_r, msg_b)[kind].at[channels[slot]], r_own.at[kind, slot, q, s], r_sem.at[4 * kind + 3]
            ).start()

    load_x[0].wait()
    lax.fori_loop(0, 3, right_rows, 0, unroll=UNROLL_PREP)
    load_x[1].wait()
    lax.fori_loop(3, 6, right_rows, 0, unroll=UNROLL_PREP)
    pack(msg_r)
    pl.semaphore_wait(barrier, 1 + 3 + 3 + 7)
    for peer in y_line:
        pl.semaphore_signal(line_y, inc=1, device_id=peer, device_id_type=MESH)
    keep_r(0)
    lax.fori_loop(0, 6, lambda k, _: send_r(0, k, (0,), (0,)), 0)
    pl.semaphore_wait(line_y, 3)
    for peer in x_line:
        pl.semaphore_signal(line_x, inc=1, device_id=peer, device_id_type=MESH)
    lax.fori_loop(0, 8, lambda k, _: send_r(0, k, (0,), (1, 2, 3)), 0)
    pl.semaphore_wait(line_x, 3)
    lax.fori_loop(0, 8, lambda k, _: send_r(0, k, (1, 2, 3), range(4)), 0)

    lax.fori_loop(0, 6, shared_rows, 0, unroll=UNROLL_PREP)
    pack(msg_b)
    keep_r(1)
    lax.fori_loop(0, 6, lambda k, _: send_r(1, k, range(4), range(4)), 0)

    def near(k, _):
        send_r(1, k, range(1, 4), range(1))
        return send_r(1, k, range(4), range(1, 4))

    lax.fori_loop(6, 8, near, 0)

    lax.fori_loop(0, 6, left_rows, 0, unroll=UNROLL_PREP)
    pack(msg_l)

    def four(zz):
        return pl.ds(((zz + NZ) % NZ) * NY, NY)

    def send_l(k, dys, dxs):
        slot, zz, d = ends(k)
        for dy in dys:
            for dx in dxs:
                pltpu.make_async_remote_copy(
                    msg_l.at[(d * NY + ys[dy]) * NX + xs[dx]], l_own.at[slot, q, s],
                    send_sem, l_sem.at[((k + 6) // 8) * 2 + slot],
                    device_id=((zz * NY + ys[dy]) * 2 + core, xs[dx]), device_id_type=MESH,
                ).start()

    rb = r_own.reshape(2 * 2 * NX * 384, 128)
    rh = r_half.reshape(2 * 2 * 384, 128)

    def to_partner(kind, source, target):
        pltpu.make_async_remote_copy(
            source, target, swap_send.at[kind], swap_sem.at[kind], device_id=other, device_id_type=MESH
        ).start()

    def to_owner(kind, n, step, source, target):
        pltpu.make_async_remote_copy(
            source, target, relay_send.at[kind], relay_sem.at[n],
            device_id=at((z + NZ + step) % NZ, y, q), device_id_type=MESH,
        ).start()

    def arrived(n):
        block = r_own.at[0, 0, 0]
        pltpu.make_async_copy(block, block, r_sem.at[n]).wait()

    sides = ((0, 1), (1, -1))

    def forward_right(n, _):
        a = 3 - n
        arrived(n)
        moves = [(slot, step, xx, four(z - a * step)) for xx in range(NX) for slot, step in sides]
        for slot, step, xx, place in moves:
            to_owner(0, n, step, r_own.at[0, slot, xx, place], r_all.at[1 - slot, xx, place, core])
        for slot, step, xx, place in moves:
            block, mine = r_own.at[0, slot, xx, place], r_all.at[slot, xx, place, core]
            to_partner(0, block, mine)
            pltpu.make_async_copy(block, mine, keep_sem.at[0]).start()
        return 0

    def forward_shared(n, _):
        a = 7 - n
        arrived(n)
        moves = []
        for pair in range(2):
            for slot, step in sides:
                zz = (z + NZ - a * step) % NZ

                def part(x):
                    start = ((2 + slot) * NX + x) * 384 + zz * 48
                    return rb[pl.ds(pl.multiple_of(start, 48), 48), :]

                rh[pl.ds(pl.multiple_of((slot * 2 + pair) * 384 + zz * 48, 48), 48), :] = jnp.concatenate(
                    [part(2 * pair)[:, 64:], part(2 * pair + 1)[:, :64]], axis=1
                )
                moves.append((slot, step, pair, pl.ds(zz * NY, NY)))
        for slot, step, pair, place in moves:
            to_owner(1, n, step, r_half.at[slot, pair, place], r_mix.at[1 - slot, pair, place, core])
        for slot, step, pair, place in moves:
            block, mine = r_half.at[slot, pair, place], r_mix.at[slot, pair, place, core]
            to_partner(1, block, mine)
            pltpu.make_async_copy(block, mine, keep_sem.at[1]).start()
        return 0

    for slot in range(2):
        pltpu.make_async_copy(msg_l.at[channels[slot]], l_own.at[slot, q, s], l_sem.at[2 + slot]).start()
    def left_to(k, _):
        send_l(k, range(4), range(4))
        return 0

    def left_near(k, _):
        send_l(k, range(1), range(1, 4))
        send_l(k, range(1, 4), range(4))
        return 0

    lax.fori_loop(0, 4, forward_right, 0)
    lax.fori_loop(4, 8, forward_shared, 0)
    lax.fori_loop(0, 4, left_to, 0)
    lax.fori_loop(4, 6, left_to, 0)
    lax.fori_loop(6, 8, left_near, 0)

    def gates(i, _):
        gate[i] = jax.nn.sigmoid(jnp.dot(normed[i], w_in[4], preferred_element_type=F32))
        return 0

    lax.fori_loop(0, ROWS, gates, 0)

    def relayed_right(n, _):
        block = r_own.at[0, 0, 0]
        pltpu.make_async_copy(block, block, relay_sem.at[n]).wait()
        for xx in range(NX):
            for slot, step in sides:
                block = r_all.at[slot, xx, four(z + (4 - n) * step), core]
                to_partner(0, block, block)
        return 0

    def relayed_shared(n, _):
        block = r_own.at[0, 0, 0, pl.ds(0, 16)]
        pltpu.make_async_copy(block, block, relay_sem.at[n]).wait()
        for pair in range(2):
            for slot, step in sides:
                block = r_mix.at[slot, pair, four(z + (8 - n) * step), core]
                to_partner(1, block, block)
        return 0

    lax.fori_loop(0, 4, relayed_right, 0)
    lax.fori_loop(4, 8, relayed_shared, 0)
    sizes = (r_own.at[0, 0], r_own.at[0, 0, pl.ds(0, 2)])
    swaps = (r_own.at[0], r_own.at[0, 0])
    for kind in range(2):
        pltpu.make_async_copy(sizes[kind], sizes[kind], keep_sem.at[kind]).wait()
        pltpu.make_async_copy(swaps[kind], swaps[kind], swap_sem.at[kind]).wait()

    ra = r_all.reshape(2 * NX * 768, 128)
    rm = r_mix.reshape(2 * 2 * 768, 128)
    la = l_own.reshape(2 * NX * 384, 128)
    whole = t_a.reshape(2 * NX * 384, 128)
    halves = t_b.reshape(2 * NX * 192, 128)

    def block(ref, n, size):
        return ref[pl.ds(pl.multiple_of(n * size, size), size), :]

    lane_b = lax.broadcasted_iota(jnp.int32, (72, 128), 1) < 64

    def rows_of(slot, which, distances):
        count = len(distances)
        places = [(z + NZ - a * (1 - 2 * slot)) % NZ for a in distances]
        channel = channels[0] - slot * (channels[0] - channels[1])
        arrived = msg_l.at[pl.ds(0, 16 * count)]
        pltpu.make_async_copy(arrived, arrived, l_sem.at[which * 2 + slot]).wait()

        def part(ref, n):
            return jnp.concatenate(
                [ref[pl.ds(pl.multiple_of(n * 384 + zz * 48, 48), 48), :] for zz in places], axis=0
            )

        lhs = [part(la, slot * NX + x) for x in range(NX)]
        for x in (0, 2):
            first = (2 + slot) * NX + x
            lhs.append(
                jnp.concatenate([part(rb, first)[:, :64], part(rb, first + 1)[:, 64:]], axis=1)
            )
        rhs = [block(ra, slot * NX + x, 768) for x in range(NX)] + [
            block(rm, slot * 2 + n, 768) for n in range(2)
        ]
        triangle = lax.dot_general(
            jnp.concatenate(lhs, axis=1), jnp.concatenate(rhs, axis=1), (((1,), (1,)), ((), ())),
            preferred_element_type=F32,
        )
        for e, zz in enumerate(places):
            for x, tile in enumerate((0, 2, 3, 5)):
                whole[pl.ds(pl.multiple_of((slot * NX + x) * 384 + zz * 48, 48), 48), :] = triangle[
                    e * 48 : (e + 1) * 48, tile * 128 : (tile + 1) * 128
                ].astype(BF16)

        def back(dy, _):
            for e, zz in enumerate(places):
                ss = zz * NY + (y + dy) % NY
                for d in range(NX):

                    def send(ss=ss, xx=xs[d]):
                        pltpu.make_async_remote_copy(
                            t_a.at[slot, xx, ss], in_a.at[channel], send_sem, a_sem,
                            device_id=(ss * 2 + core, xx), device_id_type=MESH,
                        ).start()

                    if (distances[e], d) == (0, 0):
                        pl.when(dy != 0)(send)
                    else:
                        send()
            return 0

        lax.fori_loop(0, NY, back, 0)
        for n, tile in enumerate((1, 4)):
            t_odd[n, 0 : count * 48, :] = triangle[:, tile * 128 : (tile + 1) * 128]
            even, odd = (t_odd[n, pl.ds(h, count * 24, stride=2), :] for h in range(2))
            lanes = lane_b[0 : count * 24]
            both = (
                jnp.where(lanes, even, pltpu.roll(odd, 64, 1)),
                jnp.where(lanes, pltpu.roll(even, 64, 1), odd),
            )
            for e, zz in enumerate(places):
                for h in range(2):
                    halves[pl.ds(pl.multiple_of((slot * NX + 2 * n + h) * 192 + zz * 24, 8), 24), :] = both[h][
                        e * 24 : (e + 1) * 24
                    ].astype(BF16)
        return 0

    def send_b(k, pairs):
        slot = k % 2
        zz = (z + NZ - (3 - k // 2) * (1 - 2 * slot)) % NZ
        for dy, dx in pairs:
            pltpu.make_async_remote_copy(
                t_b.at[slot, xs[dx], (zz * NY) + ys[dy]],
                in_b.at[channels[0] - slot * (channels[0] - channels[1])], send_sem, b_sem,
                device_id=((zz * NY + ys[dy]) * 2 + core, xs[dx]), device_id_type=MESH,
            ).start()
        return 0

    every = [(dy, dx) for dy in range(NY) for dx in range(NX)]
    lax.fori_loop(0, 2, lambda slot, _: rows_of(slot, 0, (3,)), 0)
    lax.fori_loop(0, 2, lambda k, _: send_b(k, every), 0)
    lax.fori_loop(0, 2, lambda slot, _: rows_of(slot, 1, (2, 1, 0)), 0)
    for slot in range(2):
        pltpu.make_async_copy(t_a.at[slot, q, s], in_a.at[channels[slot]], a_sem).start()
        pltpu.make_async_copy(t_b.at[slot, q, s], in_b.at[channels[slot]], b_sem).start()
    lax.fori_loop(2, 6, lambda k, _: send_b(k, every), 0)
    lax.fori_loop(6, 8, lambda k, _: send_b(k, every[1:]), 0)

    def unpack(source, steps):
        def some(n, _):
            rows = pl.ds(pl.multiple_of(n * 256, 256), 256)
            stage[rows, :] = source[rows, :].astype(F32)
            return 0

        lax.fori_loop(0, steps, some, 0)

    def projected(g, stride):
        scaled = unit_norm(stage[pl.ds(g, NC, stride=stride), :], 0)
        return lax.dot_general(
            scaled.astype(BF16), w_in[5], (((0,), (0,)), ((), ())), preferred_element_type=F32
        )

    a0 = pl.multiple_of((q % 2) * 64, 64)
    b0 = pl.multiple_of((1 - q % 2) * 128, 128)

    def whole_rows(i, _):
        out_ref[i, pl.ds(a0, 128), :] = (gate[i, pl.ds(a0, 128), :] * projected(i, 12)).astype(BF16)
        return 0

    def half_rows(p, _):
        both = projected(p, 6)
        for e in range(2):
            out_ref[2 * p + e, pl.ds(b0, 64), :] = (
                gate[2 * p + e, pl.ds(b0, 64), :] * both[e * 64 : (e + 1) * 64]
            ).astype(BF16)
        return 0

    pltpu.make_async_copy(in_a, in_a, a_sem).wait()
    unpack(in_a.reshape(NC * 12, 128), 6)
    lax.fori_loop(0, 12, whole_rows, 0, unroll=UNROLL)
    pltpu.make_async_copy(in_b, in_b, b_sem).wait()
    unpack(in_b.reshape(NC * 6, 128), 3)
    lax.fori_loop(0, 6, half_rows, 0, unroll=UNROLL)
    for sent in (msg_r, msg_b, msg_l, in_a, in_b):
        sent = sent.at[pl.ds(0, NC - 2)]
        pltpu.make_async_copy(sent, sent, send_sem).wait()
    for kind in range(2):
        pltpu.make_async_copy(sizes[kind], sizes[kind], relay_send.at[kind]).wait()
        pltpu.make_async_copy(swaps[kind], swaps[kind], swap_send.at[kind]).wait()


def local(*args):
    hbm = pl.BlockSpec(memory_space=pltpu.HBM)
    vmem = pl.BlockSpec(memory_space=pltpu.VMEM)
    dma = pltpu.SemaphoreType.DMA
    return pl.pallas_call(
        kernel,
        out_shape=jax.ShapeDtypeStruct((ROWS, COLS, WIDTH), BF16),
        in_specs=[hbm] * 8,
        out_specs=vmem,
        scratch_shapes=[
            pltpu.VMEM((ROWS, COLS, WIDTH), BF16),
            pltpu.SMEM((12, 12), jnp.int32),
            pltpu.VMEM((6, WIDTH, WIDTH), BF16),
            pltpu.VMEM((4 * WIDTH, WIDTH), BF16),
            pltpu.VMEM((ROWS, COLS, WIDTH), BF16),
            pltpu.VMEM((6, 384, WIDTH), BF16),
            pltpu.VMEM((ROWS, COLS, WIDTH), F32),
            pltpu.VMEM((NC * 12, 128), F32),
            pltpu.VMEM((NC, 3, 4, 128), BF16),
            pltpu.VMEM((NC, 3, 4, 128), BF16),
            pltpu.VMEM((NC, 3, 4, 128), BF16),
            pltpu.VMEM((2, 2, NX, NS, 3, 4, 128), BF16),
            pltpu.VMEM((2, NX, NS, 2, 3, 4, 128), BF16),
            pltpu.VMEM((2, 2, NS, 3, 4, 128), BF16),
            pltpu.VMEM((2, 2, NS, 2, 3, 4, 128), BF16),
            pltpu.VMEM((2, NX, NS, 3, 4, 128), BF16),
            pltpu.VMEM((2, 144, 128), F32),
            pltpu.VMEM((2, NX, NS, 6, 2, 128), BF16),
            pltpu.VMEM((2, NX, NS, 3, 2, 128), BF16),
            pltpu.VMEM((NC, 6, 2, 128), BF16),
            pltpu.VMEM((NC, 3, 2, 128), BF16),
            dma((4,)), dma, dma((2 * NX,)), dma((4,)), dma, dma,
            dma((2 * NX,)), dma((2,)), dma((2,)), dma((2,)), dma((2,)),
            pltpu.SemaphoreType.REGULAR, pltpu.SemaphoreType.REGULAR,
        ],
        compiler_params=pltpu.CompilerParams(
            collective_id=0, has_side_effects=True, vmem_limit_bytes=40 * 2**20
        ),
    )(*(pltpu.with_memory_space_constraint(a, pltpu.HBM) for a in args))


def solution(mesh):
    return jax.shard_map(
        local,
        mesh=mesh,
        in_specs=(P("row", "col", None), P(), P(), P(), P(), P(), P(), P()),
        out_specs=P("row", "col", None),
        check_vma=False,
    )
```

```python
import functools

import jax
import jax.numpy as jnp
from jax import lax
from jax.experimental import pallas as pl
from jax.experimental.pallas import tpu as pltpu
from jax.sharding import PartitionSpec as P

MESH = pl.DeviceIdType.MESH
NX, NY, NZ, NS, NC = 4, 4, 8, 32, 128
ROWS, COLS, WIDTH = 12, 192, 128
F32, BF16 = jnp.float32, jnp.bfloat16
UNROLL, UNROLL_PREP = 6, 3


def unit_norm(values, axis):
    mean = jnp.mean(values, axis=axis, keepdims=True)
    centred = values - mean
    spread = jnp.mean(centred * centred, axis=axis, keepdims=True)
    return centred * lax.rsqrt(spread + 1e-05)


def kernel(
    x_hbm, tm_hbm, wlg_hbm, wl_hbm, wrg_hbm, wr_hbm, wog_hbm, wo_hbm, out_ref,
    x_ref, tm_ref, w_in, wt, normed, masked, gate, stage, msg_r, msg_b, msg_l, r_own, r_all, r_half, r_mix, l_own,
    t_odd, t_a, t_b, in_a, in_b,
    load_sem, send_sem, r_sem, l_sem, a_sem, b_sem, relay_sem, relay_send, swap_sem, swap_send, keep_sem,
    line_y, line_x,
):
    row, q = lax.axis_index("row"), lax.axis_index("col")
    core, y, z = row % 2, (row // 2) % NY, row // (2 * NY)
    s = row // 2
    channels = [s * NX + q, (((z + NZ - 1) % NZ) * NY + y) * NX + q]
    other = ((s * 2) + 1 - core, q)

    weights = (wlg_hbm, wl_hbm, wrg_hbm, wr_hbm, wog_hbm, wo_hbm)
    for n, w in enumerate(weights):
        pltpu.make_async_copy(w, w_in.at[n], load_sem.at[0]).start()
    load_mask = pltpu.make_async_copy(tm_hbm, tm_ref, load_sem.at[1])
    load_mask.start()
    load_x = [
        pltpu.make_async_copy(x_hbm.at[pl.ds(6 * n, 6)], x_ref.at[pl.ds(6 * n, 6)], load_sem.at[2 + n])
        for n in range(2)
    ]
    for load in load_x:
        load.start()

    xs = [(q + d) % NX for d in range(NX)]
    ys = [(y + d) % NY for d in range(NY)]

    def at(zz, yy, xx):
        return ((zz * NY + yy) * 2 + core, xx)

    x_line = [at(z, y, (q + d) % NX) for d in range(1, NX)]
    y_line = [at(z, (y + d) % NY, q) for d in range(1, NY)]
    z_line = [at((z + d) % NZ, y, q) for d in (4, 3, 5, 2, 6, 1, 7)]
    barrier = pltpu.get_barrier_semaphore()
    for peer in [*z_line, *y_line, *x_line, other]:
        pl.semaphore_signal(barrier, inc=1, device_id=peer, device_id_type=MESH)

    pltpu.make_async_copy(w_in, w_in, load_sem.at[0]).wait()
    for n in range(4):
        wt[n * WIDTH : (n + 1) * WIDTH, :] = w_in[n].astype(F32).T.astype(BF16)
    low = lax.broadcasted_iota(jnp.int32, (WIDTH, 128), 1) < 64
    odd_q = q % 2 == 1
    load_mask.wait()

    def project(n, values):
        return lax.dot_general(
            wt[n * WIDTH : (n + 1) * WIDTH, :], values, (((1,), (1,)), ((), ())),
            preferred_element_type=F32,
        )

    def store(n, rows):
        stage[pl.ds(n, NC, stride=12), :] = rows

    def right_rows(p, _):
        parts = {}
        for e in range(2):
            i = 2 * p + e
            n = unit_norm(x_ref[i].astype(F32), 1)
            normed[i] = n.astype(BF16)
            tile = (row * ROWS + i) // 64
            for t in range(3):
                m = tm_ref[tile, q * 3 + t].astype(F32)
                parts[e, t] = (n[t * 64 : (t + 1) * 64] * m).astype(BF16)
        firsts = jnp.concatenate([parts[0, 0], parts[0, 1], parts[1, 0], parts[1, 1]], axis=0)
        masked[p, 0:256, :] = firsts
        masked[p, 256:384, :] = jnp.concatenate([parts[0, 2], parts[1, 2]], axis=0)
        right = jax.nn.sigmoid(project(2, firsts)) * project(3, firsts)
        for e in range(2):
            store(2 * p + e, right[:, e * 128 : (e + 1) * 128])
        return 0

    def shared_rows(p, _):
        lasts = masked[p, 256:384, :]
        right = jax.nn.sigmoid(project(2, lasts)) * project(3, lasts)
        left = jax.nn.sigmoid(project(0, lasts)) * project(1, lasts)
        first, second = jnp.where(odd_q, right, left), jnp.where(odd_q, left, right)
        store(2 * p, jnp.where(low, first, pltpu.roll(second, 64, 1)))
        store(2 * p + 1, jnp.where(low, pltpu.roll(first, 64, 1), second))
        return 0

    def left_rows(p, _):
        firsts = masked[p, 0:256, :]
        left = jax.nn.sigmoid(project(0, firsts)) * project(1, firsts)
        for e in range(2):
            store(2 * p + e, left[:, e * 128 : (e + 1) * 128])
        return 0

    def pack(message):
        target = message.reshape(NC * 12, 128)

        def some(n, _):
            rows = pl.ds(pl.multiple_of(n * 256, 256), 256)
            target[rows, :] = stage[rows, :].astype(BF16)
            return 0

        lax.fori_loop(0, 6, some, 0)

    def ends(k):
        slot = k % 2
        zz = (z + NZ + (3 - k // 2) * (1 - 2 * slot)) % NZ
        return slot, zz, (zz + NZ - slot) % NZ

    def send_r(kind, k, dxs, dys):
        slot, zz, d = ends(k)
        for dy in dys:
            for dx in dxs:
                pltpu.make_async_remote_copy(
                    (msg_r, msg_b)[kind].at[(d * NY + ys[dy]) * NX + xs[dx]],
                    r_own.at[kind, slot, q, s], send_sem, r_sem.at[4 * kind + k // 2],
                    device_id=((zz * NY + ys[dy]) * 2 + core, xs[dx]), device_id_type=MESH,
                ).start()
        return 0

    def keep_r(kind):
        for slot in range(2):
            pltpu.make_async_copy(
                (msg_r, msg_b)[kind].at[channels[slot]], r_own.at[kind, slot, q, s], r_sem.at[4 * kind + 3]
            ).start()

    load_x[0].wait()
    lax.fori_loop(0, 3, right_rows, 0, unroll=UNROLL_PREP)
    load_x[1].wait()
    lax.fori_loop(3, 6, right_rows, 0, unroll=UNROLL_PREP)
    pack(msg_r)
    pl.semaphore_wait(barrier, 1 + 3 + 3 + 7)
    for peer in y_line:
        pl.semaphore_signal(line_y, inc=1, device_id=peer, device_id_type=MESH)
    keep_r(0)
    lax.fori_loop(0, 6, lambda k, _: send_r(0, k, (0,), (0,)), 0)
    pl.semaphore_wait(line_y, 3)
    for peer in x_line:
        pl.semaphore_signal(line_x, inc=1, device_id=peer, device_id_type=MESH)
    lax.fori_loop(0, 8, lambda k, _: send_r(0, k, (0,), (1, 2, 3)), 0)
    pl.semaphore_wait(line_x, 3)
    lax.fori_loop(0, 8, lambda k, _: send_r(0, k, (1, 2, 3), range(4)), 0)

    lax.fori_loop(0, 6, shared_rows, 0, unroll=UNROLL_PREP)
    pack(msg_b)
    keep_r(1)
    lax.fori_loop(0, 6, lambda k, _: send_r(1, k, range(4), range(4)), 0)

    def near(k, _):
        send_r(1, k, range(1, 4), range(1))
        return send_r(1, k, range(4), range(1, 4))

    lax.fori_loop(6, 8, near, 0)

    lax.fori_loop(0, 6, left_rows, 0, unroll=UNROLL_PREP)
    pack(msg_l)

    def four(zz):
        return pl.ds(((zz + NZ) % NZ) * NY, NY)

    def send_l(k, dys, dxs):
        slot, zz, d = ends(k)
        for dy in dys:
            for dx in dxs:
                pltpu.make_async_remote_copy(
                    msg_l.at[(d * NY + ys[dy]) * NX + xs[dx]], l_own.at[slot, q, s],
                    send_sem, l_sem.at[((k + 6) // 8) * 2 + slot],
                    device_id=((zz * NY + ys[dy]) * 2 + core, xs[dx]), device_id_type=MESH,
                ).start()

    rb = r_own.reshape(2 * 2 * NX * 384, 128)
    rh = r_half.reshape(2 * 2 * 384, 128)

    def to_partner(kind, source, target):
        pltpu.make_async_remote_copy(
            source, target, swap_send.at[kind], swap_sem.at[kind], device_id=other, device_id_type=MESH
        ).start()

    def to_owner(kind, n, step, source, target):
        pltpu.make_async_remote_copy(
            source, target, relay_send.at[kind], relay_sem.at[n],
            device_id=at((z + NZ + step) % NZ, y, q), device_id_type=MESH,
        ).start()

    def arrived(n):
        block = r_own.at[0, 0, 0]
        pltpu.make_async_copy(block, block, r_sem.at[n]).wait()

    sides = ((0, 1), (1, -1))

    def gates(i, _):
        gate[i] = jax.nn.sigmoid(jnp.dot(normed[i], w_in[4], preferred_element_type=F32))
        return 0

    def forward_right(n, _):
        a = 3 - n
        lax.fori_loop(3 * n, 3 * n + 3, gates, 0)
        arrived(n)
        moves = [(slot, step, xx, four(z - a * step)) for xx in range(NX) for slot, step in sides]
        for slot, step, xx, place in moves:
            to_owner(0, n, step, r_own.at[0, slot, xx, place], r_all.at[1 - slot, xx, place, core])
        for slot, step, xx, place in moves:
            block, mine = r_own.at[0, slot, xx, place], r_all.at[slot, xx, place, core]
            to_partner(0, block, mine)
            pltpu.make_async_copy(block, mine, keep_sem.at[0]).start()
        return 0

    def relayed_right(n, _):
        block = r_own.at[0, 0, 0]
        pltpu.make_async_copy(block, block, relay_sem.at[n]).wait()
        for xx in range(NX):
            for slot, step in sides:
                block = r_all.at[slot, xx, four(z + (4 - n) * step), core]
                to_partner(0, block, block)
        return 0

    def forward_shared(n, _):
        a = 7 - n
        arrived(n)
        moves = []
        for pair in range(2):
            for slot, step in sides:
                zz = (z + NZ - a * step) % NZ

                def part(x):
                    start = ((2 + slot) * NX + x) * 384 + zz * 48
                    return rb[pl.ds(pl.multiple_of(start, 48), 48), :]

                rh[pl.ds(pl.multiple_of((slot * 2 + pair) * 384 + zz * 48, 48), 48), :] = jnp.concatenate(
                    [part(2 * pair)[:, 64:], part(2 * pair + 1)[:, :64]], axis=1
                )
                moves.append((slot, step, pair, pl.ds(zz * NY, NY)))
        for slot, step, pair, place in moves:
            to_owner(1, n, step, r_half.at[slot, pair, place], r_mix.at[1 - slot, pair, place, core])
        for slot, step, pair, place in moves:
            block, mine = r_half.at[slot, pair, place], r_mix.at[slot, pair, place, core]
            to_partner(1, block, mine)
            pltpu.make_async_copy(block, mine, keep_sem.at[1]).start()
        return 0

    for slot in range(2):
        pltpu.make_async_copy(msg_l.at[channels[slot]], l_own.at[slot, q, s], l_sem.at[2 + slot]).start()
    def left_to(k, _):
        send_l(k, range(4), range(4))
        return 0

    def left_near(k, _):
        send_l(k, range(1), range(1, 4))
        send_l(k, range(1, 4), range(4))
        return 0

    lax.fori_loop(0, 4, forward_right, 0)
    def both(n, _):
        forward_shared(n, 0)
        return relayed_right(n - 4, 0)

    lax.fori_loop(4, 7, both, 0)
    forward_shared(7, 0)
    lax.fori_loop(0, 4, left_to, 0)
    lax.fori_loop(4, 6, left_to, 0)
    lax.fori_loop(6, 8, left_near, 0)

    def relayed_shared(n, _):
        block = r_own.at[0, 0, 0, pl.ds(0, 16)]
        pltpu.make_async_copy(block, block, relay_sem.at[n]).wait()
        for pair in range(2):
            for slot, step in sides:
                block = r_mix.at[slot, pair, four(z + (8 - n) * step), core]
                to_partner(1, block, block)
        return 0

    relayed_right(3, 0)
    lax.fori_loop(4, 8, relayed_shared, 0)
    sizes = (r_own.at[0, 0], r_own.at[0, 0, pl.ds(0, 2)])
    swaps = (r_own.at[0], r_own.at[0, 0])
    for kind in range(2):
        pltpu.make_async_copy(sizes[kind], sizes[kind], keep_sem.at[kind]).wait()
        pltpu.make_async_copy(swaps[kind], swaps[kind], swap_sem.at[kind]).wait()

    ra = r_all.reshape(2 * NX * 768, 128)
    rm = r_mix.reshape(2 * 2 * 768, 128)
    la = l_own.reshape(2 * NX * 384, 128)
    whole = t_a.reshape(2 * NX * 384, 128)
    halves = t_b.reshape(2 * NX * 192, 128)

    def block(ref, n, size):
        return ref[pl.ds(pl.multiple_of(n * size, size), size), :]

    lane_b = lax.broadcasted_iota(jnp.int32, (72, 128), 1) < 64

    def rows_of(slot, which, distances):
        count = len(distances)
        places = [(z + NZ - a * (1 - 2 * slot)) % NZ for a in distances]
        channel = channels[0] - slot * (channels[0] - channels[1])
        arrived = msg_l.at[pl.ds(0, 16 * count)]
        pltpu.make_async_copy(arrived, arrived, l_sem.at[which * 2 + slot]).wait()

        def part(ref, n):
            return jnp.concatenate(
                [ref[pl.ds(pl.multiple_of(n * 384 + zz * 48, 48), 48), :] for zz in places], axis=0
            )

        lhs = [part(la, slot * NX + x) for x in range(NX)]
        for x in (0, 2):
            first = (2 + slot) * NX + x
            lhs.append(
                jnp.concatenate([part(rb, first)[:, :64], part(rb, first + 1)[:, 64:]], axis=1)
            )
        rhs = [block(ra, slot * NX + x, 768) for x in range(NX)] + [
            block(rm, slot * 2 + n, 768) for n in range(2)
        ]
        triangle = lax.dot_general(
            jnp.concatenate(lhs, axis=1), jnp.concatenate(rhs, axis=1), (((1,), (1,)), ((), ())),
            preferred_element_type=F32,
        )
        for e, zz in enumerate(places):
            for x, tile in enumerate((0, 2, 3, 5)):
                whole[pl.ds(pl.multiple_of((slot * NX + x) * 384 + zz * 48, 48), 48), :] = triangle[
                    e * 48 : (e + 1) * 48, tile * 128 : (tile + 1) * 128
                ].astype(BF16)

        def back(dy, _):
            for e, zz in enumerate(places):
                ss = zz * NY + (y + dy) % NY
                for d in range(NX):

                    def send(ss=ss, xx=xs[d]):
                        pltpu.make_async_remote_copy(
                            t_a.at[slot, xx, ss], in_a.at[channel], send_sem, a_sem,
                            device_id=(ss * 2 + core, xx), device_id_type=MESH,
                        ).start()

                    if (distances[e], d) == (0, 0):
                        pl.when(dy != 0)(send)
                    else:
                        send()
            return 0

        lax.fori_loop(0, NY, back, 0)
        for n, tile in enumerate((1, 4)):
            t_odd[n, 0 : count * 48, :] = triangle[:, tile * 128 : (tile + 1) * 128]
            even, odd = (t_odd[n, pl.ds(h, count * 24, stride=2), :] for h in range(2))
            lanes = lane_b[0 : count * 24]
            both = (
                jnp.where(lanes, even, pltpu.roll(odd, 64, 1)),
                jnp.where(lanes, pltpu.roll(even, 64, 1), odd),
            )
            for e, zz in enumerate(places):
                for h in range(2):
                    halves[pl.ds(pl.multiple_of((slot * NX + 2 * n + h) * 192 + zz * 24, 8), 24), :] = both[h][
                        e * 24 : (e + 1) * 24
                    ].astype(BF16)
        return 0

    def send_b(k, pairs):
        slot = k % 2
        zz = (z + NZ - (3 - k // 2) * (1 - 2 * slot)) % NZ
        for dy, dx in pairs:
            pltpu.make_async_remote_copy(
                t_b.at[slot, xs[dx], (zz * NY) + ys[dy]],
                in_b.at[channels[0] - slot * (channels[0] - channels[1])], send_sem, b_sem,
                device_id=((zz * NY + ys[dy]) * 2 + core, xs[dx]), device_id_type=MESH,
            ).start()
        return 0

    every = [(dy, dx) for dy in range(NY) for dx in range(NX)]
    lax.fori_loop(0, 2, lambda slot, _: rows_of(slot, 0, (3,)), 0)
    lax.fori_loop(0, 2, lambda k, _: send_b(k, every), 0)
    lax.fori_loop(0, 2, lambda slot, _: rows_of(slot, 1, (2, 1, 0)), 0)
    for slot in range(2):
        pltpu.make_async_copy(t_a.at[slot, q, s], in_a.at[channels[slot]], a_sem).start()
        pltpu.make_async_copy(t_b.at[slot, q, s], in_b.at[channels[slot]], b_sem).start()
    lax.fori_loop(2, 6, lambda k, _: send_b(k, every), 0)
    lax.fori_loop(6, 8, lambda k, _: send_b(k, every[1:]), 0)

    def unpack(source, steps):
        def some(n, _):
            rows = pl.ds(pl.multiple_of(n * 256, 256), 256)
            stage[rows, :] = source[rows, :].astype(F32)
            return 0

        lax.fori_loop(0, steps, some, 0)

    def projected(g, stride):
        scaled = unit_norm(stage[pl.ds(g, NC, stride=stride), :], 0)
        return lax.dot_general(
            scaled.astype(BF16), w_in[5], (((0,), (0,)), ((), ())), preferred_element_type=F32
        )

    a0 = pl.multiple_of((q % 2) * 64, 64)
    b0 = pl.multiple_of((1 - q % 2) * 128, 128)

    def whole_rows(i, _):
        out_ref[i, pl.ds(a0, 128), :] = (gate[i, pl.ds(a0, 128), :] * projected(i, 12)).astype(BF16)
        return 0

    def half_rows(p, _):
        both = projected(p, 6)
        for e in range(2):
            out_ref[2 * p + e, pl.ds(b0, 64), :] = (
                gate[2 * p + e, pl.ds(b0, 64), :] * both[e * 64 : (e + 1) * 64]
            ).astype(BF16)
        return 0

    pltpu.make_async_copy(in_a, in_a, a_sem).wait()
    unpack(in_a.reshape(NC * 12, 128), 6)
    lax.fori_loop(0, 12, whole_rows, 0, unroll=UNROLL)
    pltpu.make_async_copy(in_b, in_b, b_sem).wait()
    unpack(in_b.reshape(NC * 6, 128), 3)
    lax.fori_loop(0, 6, half_rows, 0, unroll=UNROLL)
    for sent in (msg_r, msg_b, msg_l, in_a, in_b):
        sent = sent.at[pl.ds(0, NC - 2)]
        pltpu.make_async_copy(sent, sent, send_sem).wait()
    for kind in range(2):
        pltpu.make_async_copy(sizes[kind], sizes[kind], relay_send.at[kind]).wait()
        pltpu.make_async_copy(swaps[kind], swaps[kind], swap_send.at[kind]).wait()


def local(*args):
    hbm = pl.BlockSpec(memory_space=pltpu.HBM)
    vmem = pl.BlockSpec(memory_space=pltpu.VMEM)
    dma = pltpu.SemaphoreType.DMA
    return pl.pallas_call(
        kernel,
        out_shape=jax.ShapeDtypeStruct((ROWS, COLS, WIDTH), BF16),
        in_specs=[hbm] * 8,
        out_specs=vmem,
        scratch_shapes=[
            pltpu.VMEM((ROWS, COLS, WIDTH), BF16),
            pltpu.SMEM((12, 12), jnp.int32),
            pltpu.VMEM((6, WIDTH, WIDTH), BF16),
            pltpu.VMEM((4 * WIDTH, WIDTH), BF16),
            pltpu.VMEM((ROWS, COLS, WIDTH), BF16),
            pltpu.VMEM((6, 384, WIDTH), BF16),
            pltpu.VMEM((ROWS, COLS, WIDTH), F32),
            pltpu.VMEM((NC * 12, 128), F32),
            pltpu.VMEM((NC, 3, 4, 128), BF16),
            pltpu.VMEM((NC, 3, 4, 128), BF16),
            pltpu.VMEM((NC, 3, 4, 128), BF16),
            pltpu.VMEM((2, 2, NX, NS, 3, 4, 128), BF16),
            pltpu.VMEM((2, NX, NS, 2, 3, 4, 128), BF16),
            pltpu.VMEM((2, 2, NS, 3, 4, 128), BF16),
            pltpu.VMEM((2, 2, NS, 2, 3, 4, 128), BF16),
            pltpu.VMEM((2, NX, NS, 3, 4, 128), BF16),
            pltpu.VMEM((2, 144, 128), F32),
            pltpu.VMEM((2, NX, NS, 6, 2, 128), BF16),
            pltpu.VMEM((2, NX, NS, 3, 2, 128), BF16),
            pltpu.VMEM((NC, 6, 2, 128), BF16),
            pltpu.VMEM((NC, 3, 2, 128), BF16),
            dma((4,)), dma, dma((2 * NX,)), dma((4,)), dma, dma,
            dma((2 * NX,)), dma((2,)), dma((2,)), dma((2,)), dma((2,)),
            pltpu.SemaphoreType.REGULAR, pltpu.SemaphoreType.REGULAR,
        ],
        compiler_params=pltpu.CompilerParams(
            collective_id=0, has_side_effects=True, vmem_limit_bytes=40 * 2**20
        ),
    )(*(pltpu.with_memory_space_constraint(a, pltpu.HBM) for a in args))


def solution(mesh):
    return jax.shard_map(
        local,
        mesh=mesh,
        in_specs=(P("row", "col", None), P(), P(), P(), P(), P(), P(), P()),
        out_specs=P("row", "col", None),
        check_vma=False,
    )
```

```python
import functools

import jax
import jax.numpy as jnp
from jax import lax
from jax.experimental import pallas as pl
from jax.experimental.pallas import tpu as pltpu
from jax.sharding import PartitionSpec as P

MESH = pl.DeviceIdType.MESH
NX, NY, NZ, NS, NC = 4, 4, 8, 32, 128
ROWS, COLS, WIDTH = 12, 192, 128
F32, BF16 = jnp.float32, jnp.bfloat16
UNROLL, UNROLL_PREP = 6, 3


def unit_norm(values, axis):
    mean = jnp.mean(values, axis=axis, keepdims=True)
    centred = values - mean
    spread = jnp.mean(centred * centred, axis=axis, keepdims=True)
    return centred * lax.rsqrt(spread + 1e-05)


def kernel(
    x_hbm, tm_hbm, wlg_hbm, wl_hbm, wrg_hbm, wr_hbm, wog_hbm, wo_hbm, out_ref,
    x_ref, tm_ref, w_in, wt, normed, masked, gate, stage, msg_r, msg_b, msg_l, r_own, r_all, r_half, r_mix, l_own,
    t_odd, t_a, t_b, in_a, in_b,
    load_sem, send_sem, r_sem, l_sem, a_sem, b_sem, relay_sem, relay_send, swap_sem, swap_send, keep_sem,
    line_y, line_x,
):
    row, q = lax.axis_index("row"), lax.axis_index("col")
    core, y, z = row % 2, (row // 2) % NY, row // (2 * NY)
    s = row // 2
    channels = [s * NX + q, (((z + NZ - 1) % NZ) * NY + y) * NX + q]
    other = ((s * 2) + 1 - core, q)

    weights = (wlg_hbm, wl_hbm, wrg_hbm, wr_hbm, wog_hbm, wo_hbm)
    for n, w in enumerate(weights):
        pltpu.make_async_copy(w, w_in.at[n], load_sem.at[0]).start()
    load_mask = pltpu.make_async_copy(tm_hbm, tm_ref, load_sem.at[1])
    load_mask.start()
    load_x = [
        pltpu.make_async_copy(x_hbm.at[pl.ds(6 * n, 6)], x_ref.at[pl.ds(6 * n, 6)], load_sem.at[2 + n])
        for n in range(2)
    ]
    for load in load_x:
        load.start()

    xs = [(q + d) % NX for d in range(NX)]
    ys = [(y + d) % NY for d in range(NY)]

    def at(zz, yy, xx):
        return ((zz * NY + yy) * 2 + core, xx)

    x_line = [at(z, y, (q + d) % NX) for d in range(1, NX)]
    y_line = [at(z, (y + d) % NY, q) for d in range(1, NY)]
    z_line = [at((z + d) % NZ, y, q) for d in (4, 3, 5, 2, 6, 1, 7)]
    barrier = pltpu.get_barrier_semaphore()
    for peer in [*z_line, *y_line, *x_line, other]:
        pl.semaphore_signal(barrier, inc=1, device_id=peer, device_id_type=MESH)

    pltpu.make_async_copy(w_in, w_in, load_sem.at[0]).wait()
    for n in range(4):
        wt[n * WIDTH : (n + 1) * WIDTH, :] = w_in[n].astype(F32).T.astype(BF16)
    low = lax.broadcasted_iota(jnp.int32, (WIDTH, 128), 1) < 64
    odd_q = q % 2 == 1
    load_mask.wait()

    def project(n, values):
        return lax.dot_general(
            wt[n * WIDTH : (n + 1) * WIDTH, :], values, (((1,), (1,)), ((), ())),
            preferred_element_type=F32,
        )

    def store(n, rows):
        stage[pl.ds(n, NC, stride=12), :] = rows

    def right_rows(p, _):
        parts = {}
        for e in range(2):
            i = 2 * p + e
            n = unit_norm(x_ref[i].astype(F32), 1)
            normed[i] = n.astype(BF16)
            tile = (row * ROWS + i) // 64
            for t in range(3):
                m = tm_ref[tile, q * 3 + t].astype(F32)
                parts[e, t] = (n[t * 64 : (t + 1) * 64] * m).astype(BF16)
        firsts = jnp.concatenate([parts[0, 0], parts[0, 1], parts[1, 0], parts[1, 1]], axis=0)
        masked[p, 0:256, :] = firsts
        masked[p, 256:384, :] = jnp.concatenate([parts[0, 2], parts[1, 2]], axis=0)
        right = jax.nn.sigmoid(project(2, firsts)) * project(3, firsts)
        for e in range(2):
            store(2 * p + e, right[:, e * 128 : (e + 1) * 128])
        return 0

    def shared_rows(p, _):
        lasts = masked[p, 256:384, :]
        right = jax.nn.sigmoid(project(2, lasts)) * project(3, lasts)
        left = jax.nn.sigmoid(project(0, lasts)) * project(1, lasts)
        first, second = jnp.where(odd_q, right, left), jnp.where(odd_q, left, right)
        store(2 * p, jnp.where(low, first, pltpu.roll(second, 64, 1)))
        store(2 * p + 1, jnp.where(low, pltpu.roll(first, 64, 1), second))
        return 0

    def left_rows(p, _):
        firsts = masked[p, 0:256, :]
        left = jax.nn.sigmoid(project(0, firsts)) * project(1, firsts)
        for e in range(2):
            store(2 * p + e, left[:, e * 128 : (e + 1) * 128])
        return 0

    def pack(message):
        target = message.reshape(NC * 12, 128)

        def some(n, _):
            rows = pl.ds(pl.multiple_of(n * 256, 256), 256)
            target[rows, :] = stage[rows, :].astype(BF16)
            return 0

        lax.fori_loop(0, 6, some, 0)

    def ends(k):
        slot = k % 2
        zz = (z + NZ + (3 - k // 2) * (1 - 2 * slot)) % NZ
        return slot, zz, (zz + NZ - slot) % NZ

    def send_r(kind, k, dxs, dys):
        slot, zz, d = ends(k)
        for dy in dys:
            for dx in dxs:
                pltpu.make_async_remote_copy(
                    (msg_r, msg_b)[kind].at[(d * NY + ys[dy]) * NX + xs[dx]],
                    r_own.at[kind, slot, q, s], send_sem, r_sem.at[4 * kind + k // 2],
                    device_id=((zz * NY + ys[dy]) * 2 + core, xs[dx]), device_id_type=MESH,
                ).start()
        return 0

    def keep_r(kind):
        for slot in range(2):
            pltpu.make_async_copy(
                (msg_r, msg_b)[kind].at[channels[slot]], r_own.at[kind, slot, q, s], r_sem.at[4 * kind + 3]
            ).start()

    load_x[0].wait()
    lax.fori_loop(0, 3, right_rows, 0, unroll=UNROLL_PREP)
    load_x[1].wait()
    lax.fori_loop(3, 6, right_rows, 0, unroll=UNROLL_PREP)
    pack(msg_r)
    pl.semaphore_wait(barrier, 1 + 3 + 3 + 7)
    for peer in y_line:
        pl.semaphore_signal(line_y, inc=1, device_id=peer, device_id_type=MESH)
    keep_r(0)
    lax.fori_loop(0, 6, lambda k, _: send_r(0, k, (0,), (0,)), 0)
    pl.semaphore_wait(line_y, 3)
    for peer in x_line:
        pl.semaphore_signal(line_x, inc=1, device_id=peer, device_id_type=MESH)
    lax.fori_loop(0, 8, lambda k, _: send_r(0, k, (0,), (1, 2, 3)), 0)
    pl.semaphore_wait(line_x, 3)
    lax.fori_loop(0, 8, lambda k, _: send_r(0, k, (1, 2, 3), range(4)), 0)

    lax.fori_loop(0, 6, shared_rows, 0, unroll=UNROLL_PREP)
    pack(msg_b)
    keep_r(1)
    lax.fori_loop(0, 6, lambda k, _: send_r(1, k, range(4), range(4)), 0)

    def near(k, _):
        send_r(1, k, range(1, 4), range(1))
        return send_r(1, k, range(4), range(1, 4))

    lax.fori_loop(6, 8, near, 0)

    lax.fori_loop(0, 6, left_rows, 0, unroll=UNROLL_PREP)
    pack(msg_l)

    def four(zz):
        return pl.ds(((zz + NZ) % NZ) * NY, NY)

    def send_l(k, dys, dxs):
        slot, zz, d = ends(k)
        for dy in dys:
            for dx in dxs:
                pltpu.make_async_remote_copy(
                    msg_l.at[(d * NY + ys[dy]) * NX + xs[dx]], l_own.at[slot, q, s],
                    send_sem, l_sem.at[((k + 6) // 8) * 2 + slot],
                    device_id=((zz * NY + ys[dy]) * 2 + core, xs[dx]), device_id_type=MESH,
                ).start()

    rb = r_own.reshape(2 * 2 * NX * 384, 128)
    rh = r_half.reshape(2 * 2 * 384, 128)

    def to_partner(kind, source, target):
        pltpu.make_async_remote_copy(
            source, target, swap_send.at[kind], swap_sem.at[kind], device_id=other, device_id_type=MESH
        ).start()

    def to_owner(kind, n, step, source, target):
        pltpu.make_async_remote_copy(
            source, target, relay_send.at[kind], relay_sem.at[n],
            device_id=at((z + NZ + step) % NZ, y, q), device_id_type=MESH,
        ).start()

    def arrived(n):
        block = r_own.at[0, 0, 0]
        pltpu.make_async_copy(block, block, r_sem.at[n]).wait()

    sides = ((0, 1), (1, -1))

    def gates(i, _):
        gate[i] = jax.nn.sigmoid(jnp.dot(normed[i], w_in[4], preferred_element_type=F32))
        return 0

    def forward_right(n, _):
        a = 3 - n
        lax.fori_loop(3 * n, 3 * n + 3, gates, 0)
        arrived(n)
        moves = [(slot, step, xx, four(z - a * step)) for xx in range(NX) for slot, step in sides]
        for slot, step, xx, place in moves:
            to_owner(0, n, step, r_own.at[0, slot, xx, place], r_all.at[1 - slot, xx, place, core])
        for slot, step, xx, place in moves:
            block, mine = r_own.at[0, slot, xx, place], r_all.at[slot, xx, place, core]
            to_partner(0, block, mine)
            pltpu.make_async_copy(block, mine, keep_sem.at[0]).start()
        return 0

    def relayed_right(n, _):
        block = r_own.at[0, 0, 0]
        pltpu.make_async_copy(block, block, relay_sem.at[n]).wait()
        for xx in range(NX):
            for slot, step in sides:
                block = r_all.at[slot, xx, four(z + (4 - n) * step), core]
                to_partner(0, block, block)
        return 0

    def forward_shared(n, _):
        a = 7 - n
        arrived(n)
        moves = []
        for pair in range(2):
            for slot, step in sides:
                zz = (z + NZ - a * step) % NZ

                def part(x):
                    start = ((2 + slot) * NX + x) * 384 + zz * 48
                    return rb[pl.ds(pl.multiple_of(start, 48), 48), :]

                rh[pl.ds(pl.multiple_of((slot * 2 + pair) * 384 + zz * 48, 48), 48), :] = jnp.concatenate(
                    [part(2 * pair)[:, 64:], part(2 * pair + 1)[:, :64]], axis=1
                )
                moves.append((slot, step, pair, pl.ds(zz * NY, NY)))
        for slot, step, pair, place in moves:
            to_owner(1, n, step, r_half.at[slot, pair, place], r_mix.at[1 - slot, pair, place, core])
        for slot, step, pair, place in moves:
            block, mine = r_half.at[slot, pair, place], r_mix.at[slot, pair, place, core]
            to_partner(1, block, mine)
            pltpu.make_async_copy(block, mine, keep_sem.at[1]).start()
        return 0

    for slot in range(2):
        pltpu.make_async_copy(msg_l.at[channels[slot]], l_own.at[slot, q, s], l_sem.at[2 + slot]).start()
    def left_to(k, _):
        send_l(k, range(4), range(4))
        return 0

    def left_near(k, _):
        send_l(k, range(1), range(1, 4))
        send_l(k, range(1, 4), range(4))
        return 0

    lax.fori_loop(0, 4, forward_right, 0)
    def both(n, _):
        forward_shared(n, 0)
        return relayed_right(n - 4, 0)

    lax.fori_loop(4, 7, both, 0)
    forward_shared(7, 0)
    lax.fori_loop(0, 4, left_to, 0)
    lax.fori_loop(4, 6, left_to, 0)
    lax.fori_loop(6, 8, left_near, 0)

    def relayed_shared(n, _):
        block = r_own.at[0, 0, 0, pl.ds(0, 16)]
        pltpu.make_async_copy(block, block, relay_sem.at[n]).wait()
        for pair in range(2):
            for slot, step in sides:
                block = r_mix.at[slot, pair, four(z + (8 - n) * step), core]
                to_partner(1, block, block)
        return 0

    relayed_right(3, 0)
    lax.fori_loop(4, 8, relayed_shared, 0)
    sizes = (r_own.at[0, 0], r_own.at[0, 0, pl.ds(0, 2)])
    swaps = (r_own.at[0], r_own.at[0, 0])
    for kind in range(2):
        pltpu.make_async_copy(sizes[kind], sizes[kind], keep_sem.at[kind]).wait()
        pltpu.make_async_copy(swaps[kind], swaps[kind], swap_sem.at[kind]).wait()

    ra = r_all.reshape(2 * NX * 768, 128)
    rm = r_mix.reshape(2 * 2 * 768, 128)
    la = l_own.reshape(2 * NX * 384, 128)
    whole = t_a.reshape(2 * NX * 384, 128)
    halves = t_b.reshape(2 * NX * 192, 128)

    def block(ref, n, size):
        return ref[pl.ds(pl.multiple_of(n * size, size), size), :]

    lane_b = lax.broadcasted_iota(jnp.int32, (72, 128), 1) < 64

    def rows_of(slot, which, distances):
        count = len(distances)
        places = [(z + NZ - a * (1 - 2 * slot)) % NZ for a in distances]
        channel = channels[0] - slot * (channels[0] - channels[1])
        arrived = msg_l.at[pl.ds(0, 16 * count)]
        pltpu.make_async_copy(arrived, arrived, l_sem.at[which * 2 + slot]).wait()

        def part(ref, n):
            return jnp.concatenate(
                [ref[pl.ds(pl.multiple_of(n * 384 + zz * 48, 48), 48), :] for zz in places], axis=0
            )

        lhs = [part(la, slot * NX + x) for x in range(NX)]
        for x in (0, 2):
            first = (2 + slot) * NX + x
            lhs.append(
                jnp.concatenate([part(rb, first)[:, :64], part(rb, first + 1)[:, 64:]], axis=1)
            )
        rhs = [block(ra, slot * NX + x, 768) for x in range(NX)] + [
            block(rm, slot * 2 + n, 768) for n in range(2)
        ]
        triangle = lax.dot_general(
            jnp.concatenate(lhs, axis=1), jnp.concatenate(rhs, axis=1), (((1,), (1,)), ((), ())),
            preferred_element_type=F32,
        )
        for e, zz in enumerate(places):
            for x, tile in enumerate((0, 2, 3, 5)):
                whole[pl.ds(pl.multiple_of((slot * NX + x) * 384 + zz * 48, 48), 48), :] = triangle[
                    e * 48 : (e + 1) * 48, tile * 128 : (tile + 1) * 128
                ].astype(BF16)

        def back(dy, _):
            for e, zz in enumerate(places):
                ss = zz * NY + (y + dy) % NY
                for d in range(NX):

                    def send(ss=ss, xx=xs[d]):
                        pltpu.make_async_remote_copy(
                            t_a.at[slot, xx, ss], in_a.at[channel], send_sem, a_sem,
                            device_id=(ss * 2 + core, xx), device_id_type=MESH,
                        ).start()

                    if (distances[e], d) == (0, 0):
                        pl.when(dy != 0)(send)
                    else:
                        send()
            return 0

        lax.fori_loop(0, NY, back, 0)
        for n, tile in enumerate((1, 4)):
            t_odd[n, 0 : count * 48, :] = triangle[:, tile * 128 : (tile + 1) * 128]
            even, odd = (t_odd[n, pl.ds(h, count * 24, stride=2), :] for h in range(2))
            lanes = lane_b[0 : count * 24]
            both = (
                jnp.where(lanes, even, pltpu.roll(odd, 64, 1)),
                jnp.where(lanes, pltpu.roll(even, 64, 1), odd),
            )
            for e, zz in enumerate(places):
                for h in range(2):
                    halves[pl.ds(pl.multiple_of((slot * NX + 2 * n + h) * 192 + zz * 24, 8), 24), :] = both[h][
                        e * 24 : (e + 1) * 24
                    ].astype(BF16)
        return 0

    def send_b(k, pairs):
        slot = k % 2
        zz = (z + NZ - (3 - k // 2) * (1 - 2 * slot)) % NZ
        for dy, dx in pairs:
            pltpu.make_async_remote_copy(
                t_b.at[slot, xs[dx], (zz * NY) + ys[dy]],
                in_b.at[channels[0] - slot * (channels[0] - channels[1])], send_sem, b_sem,
                device_id=((zz * NY + ys[dy]) * 2 + core, xs[dx]), device_id_type=MESH,
            ).start()
        return 0

    every = [(dy, dx) for dy in range(NY) for dx in range(NX)]
    def farthest(slot, _):
        rows_of(slot, 0, (3,))
        return send_b(slot, every)

    lax.fori_loop(0, 2, farthest, 0)
    lax.fori_loop(0, 2, lambda slot, _: rows_of(slot, 1, (2, 1, 0)), 0)
    for slot in range(2):
        pltpu.make_async_copy(t_a.at[slot, q, s], in_a.at[channels[slot]], a_sem).start()
        pltpu.make_async_copy(t_b.at[slot, q, s], in_b.at[channels[slot]], b_sem).start()
    lax.fori_loop(2, 6, lambda k, _: send_b(k, every), 0)
    lax.fori_loop(6, 8, lambda k, _: send_b(k, every[1:]), 0)

    def unpack(source, steps):
        def some(n, _):
            rows = pl.ds(pl.multiple_of(n * 256, 256), 256)
            stage[rows, :] = source[rows, :].astype(F32)
            return 0

        lax.fori_loop(0, steps, some, 0)

    def projected(g, stride):
        scaled = unit_norm(stage[pl.ds(g, NC, stride=stride), :], 0)
        return lax.dot_general(
            scaled.astype(BF16), w_in[5], (((0,), (0,)), ((), ())), preferred_element_type=F32
        )

    a0 = pl.multiple_of((q % 2) * 64, 64)
    b0 = pl.multiple_of((1 - q % 2) * 128, 128)

    def whole_rows(i, _):
        out_ref[i, pl.ds(a0, 128), :] = (gate[i, pl.ds(a0, 128), :] * projected(i, 12)).astype(BF16)
        return 0

    def half_rows(p, _):
        both = projected(p, 6)
        for e in range(2):
            out_ref[2 * p + e, pl.ds(b0, 64), :] = (
                gate[2 * p + e, pl.ds(b0, 64), :] * both[e * 64 : (e + 1) * 64]
            ).astype(BF16)
        return 0

    pltpu.make_async_copy(in_a, in_a, a_sem).wait()
    unpack(in_a.reshape(NC * 12, 128), 6)
    lax.fori_loop(0, 12, whole_rows, 0, unroll=UNROLL)
    pltpu.make_async_copy(in_b, in_b, b_sem).wait()
    unpack(in_b.reshape(NC * 6, 128), 3)
    lax.fori_loop(0, 6, half_rows, 0, unroll=UNROLL)
    for sent in (msg_r, msg_b, msg_l, in_a, in_b):
        sent = sent.at[pl.ds(0, NC - 2)]
        pltpu.make_async_copy(sent, sent, send_sem).wait()
    for kind in range(2):
        pltpu.make_async_copy(sizes[kind], sizes[kind], relay_send.at[kind]).wait()
        pltpu.make_async_copy(swaps[kind], swaps[kind], swap_send.at[kind]).wait()


def local(*args):
    hbm = pl.BlockSpec(memory_space=pltpu.HBM)
    vmem = pl.BlockSpec(memory_space=pltpu.VMEM)
    dma = pltpu.SemaphoreType.DMA
    return pl.pallas_call(
        kernel,
        out_shape=jax.ShapeDtypeStruct((ROWS, COLS, WIDTH), BF16),
        in_specs=[hbm] * 8,
        out_specs=vmem,
        scratch_shapes=[
            pltpu.VMEM((ROWS, COLS, WIDTH), BF16),
            pltpu.SMEM((12, 12), jnp.int32),
            pltpu.VMEM((6, WIDTH, WIDTH), BF16),
            pltpu.VMEM((4 * WIDTH, WIDTH), BF16),
            pltpu.VMEM((ROWS, COLS, WIDTH), BF16),
            pltpu.VMEM((6, 384, WIDTH), BF16),
            pltpu.VMEM((ROWS, COLS, WIDTH), F32),
            pltpu.VMEM((NC * 12, 128), F32),
            pltpu.VMEM((NC, 3, 4, 128), BF16),
            pltpu.VMEM((NC, 3, 4, 128), BF16),
            pltpu.VMEM((NC, 3, 4, 128), BF16),
            pltpu.VMEM((2, 2, NX, NS, 3, 4, 128), BF16),
            pltpu.VMEM((2, NX, NS, 2, 3, 4, 128), BF16),
            pltpu.VMEM((2, 2, NS, 3, 4, 128), BF16),
            pltpu.VMEM((2, 2, NS, 2, 3, 4, 128), BF16),
            pltpu.VMEM((2, NX, NS, 3, 4, 128), BF16),
            pltpu.VMEM((2, 144, 128), F32),
            pltpu.VMEM((2, NX, NS, 6, 2, 128), BF16),
            pltpu.VMEM((2, NX, NS, 3, 2, 128), BF16),
            pltpu.VMEM((NC, 6, 2, 128), BF16),
            pltpu.VMEM((NC, 3, 2, 128), BF16),
            dma((4,)), dma, dma((2 * NX,)), dma((4,)), dma, dma,
            dma((2 * NX,)), dma((2,)), dma((2,)), dma((2,)), dma((2,)),
            pltpu.SemaphoreType.REGULAR, pltpu.SemaphoreType.REGULAR,
        ],
        compiler_params=pltpu.CompilerParams(
            collective_id=0, has_side_effects=True, vmem_limit_bytes=40 * 2**20
        ),
    )(*(pltpu.with_memory_space_constraint(a, pltpu.HBM) for a in args))


def solution(mesh):
    return jax.shard_map(
        local,
        mesh=mesh,
        in_specs=(P("row", "col", None), P(), P(), P(), P(), P(), P(), P()),
        out_specs=P("row", "col", None),
        check_vma=False,
    )
```
